256 devices in a mesh: tm: 128 (over x, y, z), rep: 2 (over core).
Axes of the slice: x: 4, y: 4, z: 8, core: 2. Of those that a mesh axis runs over, the one named last changes fastest.
Arguments:
- rows: float32 [524288, 256], P('tm', 'rep'), may hold values from -90 to 90, as said below
- row_mask: int32 [524288], P('tm'), may hold values from 0 to 1, as said below
- key_bucket: int32 [524288], P('tm'), may hold values from 0 to 127
- gain: float32 [256], P('rep'), may hold values from 0.1 to 1.9
Outputs:
- keyed: float32 [393216, 256], P('tm', 'rep')
The draws below stay inside these ranges and needn't reach their ends.
Inputs may be any that keep to these rules, and one draw needn't show every extreme that they name: `rows`: scale per column differs; entries stay in the range. `row_mask`: of the 4096 rows of each index of tm, at least 2048 pass. Among the passing rows of one index of tm, no key bucket occurs more than 24 times, and one bucket, the same for all indices, occurs exactly 24 times on every index.
All inputs are finite; a program needn't handle non-finite values.
Results may differ from the reference program's by a relative error of at most 0.0003.
Values sent between devices are 32-bit elements; how exact they have to be, the bound alone decides.
A program may use at most 64 MiB of HBM per device.

```python
import math
import jax
import jax.numpy as jnp
from jax import lax

F = 256
WINDOW = 512
ROWS_DEV = 4096
TOTAL = 524288
MOST = 24
N_TM = 128


def draw_rows(key, part):
    kcol, kval = jax.random.split(jax.random.fold_in(key, 11), 2)
    column = jnp.exp(jax.random.uniform(kcol, (F,), jnp.float32, 0.0, math.log(10.0)))
    base = jnp.clip(jax.random.normal(kval, (TOTAL, F), jnp.float32), -6.0, 6.0)
    return base * column[None, :]


def mask_and_keys(key):
    base = jax.random.fold_in(key, 29)
    khot, kperm, kdev = jax.random.split(base, 3)
    hot = jax.random.randint(khot, (), 0, N_TM)
    relabel = jax.random.permutation(kperm, N_TM - 1).astype(jnp.int32)
    device_keys = jax.random.split(kdev, N_TM)

    def one_device(dkey):
        ka, kb, kc, kd, ke, kf, kg = jax.random.split(dkey, 7)
        places = jnp.arange(ROWS_DEV, dtype=jnp.int32)
        rate = jax.random.randint(ka, (), 0, 61)
        raw = jax.random.randint(kb, (ROWS_DEV,), 0, 100) < rate
        phase = jax.random.randint(kc, (), 0, 2)
        forced = places % 2 == phase
        start = jax.random.randint(kd, (), 0, ROWS_DEV - MOST + 1)
        inrun = (places >= start) & (places < start + MOST)
        offset = jax.random.randint(ke, (), 0, N_TM - 1)
        spread = (places // 2 + offset) % (N_TM - 1)
        picked = jnp.minimum(jax.random.randint(kf, (ROWS_DEV,), 0, N_TM - 1), jax.random.randint(kg, (ROWS_DEV,), 0, N_TM - 1))
        other = jnp.where(forced, spread, relabel[picked])
        bucket = jnp.where(other >= hot, other + 1, other)
        bucket = jnp.where(inrun, hot, bucket).astype(jnp.int32)
        live = inrun | forced | raw
        sortkey = jnp.where(live, bucket * 2 + jnp.where(inrun | forced, 0, 1), 2 * N_TM).astype(jnp.int32)
        order = jnp.argsort(sortkey, stable=True).astype(jnp.int32)
        ordered = sortkey[order]
        first = jnp.searchsorted(ordered, ordered // 2 * 2, side='left').astype(jnp.int32)
        rank = jnp.zeros((ROWS_DEV,), jnp.int32).at[order].set(places - first)
        keep = live & (rank < MOST)
        return (keep.astype(jnp.int32), bucket)
    masks, buckets = jax.vmap(one_device)(device_keys)
    return (masks.reshape(-1), buckets.reshape(-1))


def draw_row_mask(key, part):
    return mask_and_keys(key)[0]


def draw_key_bucket(key, part):
    return mask_and_keys(key)[1]


def setup_inputs(seed: int = 0) -> dict:
    key_list = jax.random.split(jax.random.key(seed), 5)
    rows = draw_rows(jax.random.fold_in(key_list[4], 71), 0)
    row_mask = draw_row_mask(jax.random.fold_in(key_list[4], 71), 0)
    key_bucket = draw_key_bucket(jax.random.fold_in(key_list[4], 71), 0)
    gain = jnp.clip(1.0 + 0.18 * jax.random.normal(key_list[3], (F,), jnp.float32), 0.1, 1.9)
    return {"rows": rows, "row_mask": row_mask, "key_bucket": key_bucket, "gain": gain}


epsilon = 1e-06

def window_sums(extended, width):
    blocks = extended.reshape(-1, width, extended.shape[1])
    inner = jnp.cumsum(blocks, axis=1)
    totals = inner[:, -1:, :]
    result = inner[1:] + totals[:-1] - inner[:-1]
    return result.reshape(-1, extended.shape[1])

def reference(rows, row_mask, key_bucket, gain):
    total_rows = rows.shape[0]
    capacity = N_TM * MOST
    positions = jnp.arange(total_rows, dtype=jnp.int32)
    live = row_mask == 1
    order_rank = (jnp.cumsum(row_mask) - 1).astype(jnp.int32)
    count = jnp.sum(row_mask).astype(jnp.int32)
    target = jnp.where(live, order_rank, total_rows).astype(jnp.int32)
    source = jnp.zeros((total_rows,), jnp.int32).at[target].set(positions, mode='drop')
    valid = positions < count
    compact = jnp.where(valid[:, None], rows[source], jnp.float32(0.0))
    compact_key = jnp.where(valid, key_bucket[source], N_TM).astype(jnp.int32)
    tail = lax.dynamic_slice_in_dim(compact, (count - WINDOW).astype(jnp.int32), WINDOW, 0)
    extended = jnp.concatenate([tail, compact], axis=0)
    sums = window_sums(extended, WINDOW)
    meansq = lax.optimization_barrier(jnp.mean(sums * sums, axis=1, keepdims=True))
    normed = sums * gain[None, :] / jnp.sqrt(meansq + epsilon)
    order = jnp.argsort(compact_key, stable=True).astype(jnp.int32)
    ordered = compact_key[order]
    first = jnp.searchsorted(ordered, ordered, side='left').astype(jnp.int32)
    placed = positions - first
    bucket_rank = jnp.zeros((total_rows,), jnp.int32).at[order].set(placed)
    dest = jnp.where(valid, compact_key * capacity + bucket_rank, N_TM * capacity).astype(jnp.int32)
    keyed = jnp.zeros((N_TM * capacity, rows.shape[1]), jnp.float32).at[dest].set(normed, mode='drop')
    return keyed
```

```python
import functools

import jax
import jax.numpy as jnp
from jax import lax
from jax.experimental import pallas as pl
from jax.experimental.pallas import tpu as pltpu
from jax.sharding import PartitionSpec as P

F = 256
WINDOW = 512
LANES = 128
EPSILON = 1e-06
MESH = pl.DeviceIdType.MESH

BIAS = 32768
INSIDE = WINDOW - BIAS
NOT_LIVE = 16384
EMPTY_SLOT = 16384
EMPTY = 1e9
LIMIT = 1e8


def iota(shape, dim):
    return lax.broadcasted_iota(jnp.int32, shape, dim)


def as_bf16(test):
    return jnp.where(test, jnp.float32(1.0), jnp.float32(0.0)).astype(jnp.bfloat16)


def ones_where(test):
    return jnp.where(test, jnp.bfloat16(1.0), jnp.bfloat16(0.0))


def mm(a, b):
    return jnp.dot(a, b, preferred_element_type=jnp.float32)


def index_kernel(most, rows_ref, mask_ref, key_ref, tail_ref, xcat_ref, crow_ref, cs_ref, empty_ref, x_ref, hits_ref, picks_ref, sem):
    size_rows = rows_ref.shape[0]
    chunks = size_rows // LANES
    load = pltpu.make_async_copy(rows_ref, x_ref, sem)
    load.start()
    mask = mask_ref[...]
    live = mask == 1
    mask_bf = mask.astype(jnp.float32).astype(jnp.bfloat16)
    upper = as_bf16(iota((LANES, LANES), 0) <= iota((LANES, LANES), 1))
    within = mm(mask_bf, upper)
    totals = mm(mask_bf, jnp.ones((LANES, LANES), jnp.bfloat16))
    below = as_bf16(iota((chunks, chunks), 1) < iota((chunks, chunks), 0))
    before = mm(below, totals.astype(jnp.bfloat16))
    count = (before + totals)[chunks - 1 : chunks, :].astype(jnp.int32)
    c = (within + before - 1.0).astype(jnp.int32)
    marked = jnp.where(live, c, NOT_LIVE)
    for a in range(chunks):
        crow_ref[a] = jnp.broadcast_to(marked[a : a + 1, :], (16, LANES)).astype(jnp.int16)
    key = jnp.where(live, key_ref[...], -1)
    buckets = iota((LANES, LANES), 0)
    for a in range(chunks):
        hits_ref[:, a * LANES : (a + 1) * LANES] = as_bf16(jnp.broadcast_to(key[a : a + 1, :], (LANES, LANES)) == buckets)
    upper2 = as_bf16(iota((256, 256), 0) <= iota((256, 256), 1))
    carry = jnp.zeros((LANES, 1), jnp.float32)
    ranks = iota((32, LANES), 0)
    for b in range(chunks // 2):
        hits = hits_ref[:, b * 256 : (b + 1) * 256]
        running = mm(hits, upper2)
        rank = jnp.sum(hits.astype(jnp.float32) * (running + carry), axis=0, keepdims=True) - 1.0
        carry = carry + running[:, 255:256]
        for h in range(2):
            a = 2 * b + h
            same = jnp.broadcast_to(rank[:, h * LANES : (h + 1) * LANES], (32, LANES)).astype(jnp.int32) == ranks
            high = jnp.broadcast_to((c[a : a + 1, :] >> 6).astype(jnp.float32), (32, LANES))
            low = jnp.broadcast_to((c[a : a + 1, :] & 63).astype(jnp.float32), (32, LANES))
            place = slice(a * LANES, (a + 1) * LANES)
            picks_ref[0:32, place] = jnp.where(same, high, 0.0).astype(jnp.bfloat16)
            picks_ref[32:64, place] = jnp.where(same, low, 0.0).astype(jnp.bfloat16)
            picks_ref[64:96, place] = jnp.where(same, 1.0, 0.0).astype(jnp.bfloat16)
    found = lax.dot_general(picks_ref[...], hits_ref[...], (((1,), (1,)), ((), ())), preferred_element_type=jnp.float32)
    filled = found[64:96, :] > 0.5
    slots = found[0:32, :] * 64.0 + found[32:64, :]
    slots = jnp.where(filled, slots.astype(jnp.int32) - BIAS, EMPTY_SLOT)
    empty_ref[...] = jnp.where(filled, 0.0, EMPTY)[:most, :]
    for k in range(0, LANES, 2):
        pair = [jnp.broadcast_to(slots[:most, k + j : k + j + 1], (most, LANES)) for j in range(2)]
        cs_ref[k * most : (k + 2) * most, :] = jnp.concatenate(pair, axis=0).astype(jnp.int16)
    load.wait()
    x = x_ref[...]
    high = x.astype(jnp.bfloat16)
    xcat_ref[:, :LANES] = high
    xcat_ref[:, LANES:] = (x - high.astype(jnp.float32)).astype(jnp.bfloat16)
    wanted = jnp.broadcast_to(count - WINDOW, (WINDOW, LANES)) + iota((WINDOW, LANES), 0)
    wanted = wanted.astype(jnp.int16)
    first = (size_rows // 2 - WINDOW) // LANES
    parts = []
    for a in range(first, chunks):
        parts.append(ones_where(wanted == jnp.broadcast_to(crow_ref[a][None], (WINDOW // 16, 16, LANES)).reshape(WINDOW, LANES)))
    both = mm(jnp.concatenate(parts, axis=1), xcat_ref[first * LANES :, :])
    tail_ref[...] = both[:, :LANES] + both[:, LANES:]


def own_kernel(block, xcat_ref, crow_ref, cs_ref, sums_ref, w_ref):
    chunks = crow_ref.shape[0]

    def step(m, carry):
        base = pl.multiple_of(m * block, block)
        for t in range(block // 16):
            cs = cs_ref[pl.ds(base + t * 16, 16), :]
            for a in range(chunks):
                w_ref[t * 16 : (t + 1) * 16, a * LANES : (a + 1) * LANES] = ones_where(cs - crow_ref[a] < INSIDE)
        both = mm(w_ref[...], xcat_ref[...])
        sums_ref[pl.ds(base, block), :] = both[:, :LANES] + both[:, LANES:]
        return carry

    lax.fori_loop(0, cs_ref.shape[0] // block, step, 0)


def tail_kernel(most, sums_ref, tail_ref, cs_ref, y_ref, sq_ref):
    tail = tail_ref[...]
    high = tail.astype(jnp.bfloat16)
    tailcat = jnp.concatenate([high, (tail - high.astype(jnp.float32)).astype(jnp.bfloat16)], axis=1)
    lanes = iota((most, LANES), 1)
    group = 16
    size = group * most

    def add_tail(j, sq):
        base = pl.multiple_of(j * size, size)
        cs = cs_ref[pl.ds(base, size), :]
        parts = [
            ones_where(cs - (iota((size, LANES), 1) + (a * LANES - WINDOW)).astype(jnp.int16) < INSIDE) for a in range(WINDOW // LANES)
        ]
        both = mm(jnp.concatenate(parts, axis=1), tailcat)
        y = sums_ref[pl.ds(base, size), :] + both[:, :LANES] + both[:, LANES:]
        y_ref[pl.ds(base, size), :] = y
        squares = jnp.sum(y * y, axis=1, keepdims=True)
        for i in range(group):
            sq = jnp.where(lanes == j * group + i, squares[i * most : (i + 1) * most, :], sq)
        return sq

    sq_ref[...] = lax.fori_loop(0, y_ref.shape[0] // size, add_tail, jnp.zeros((most, LANES), jnp.float32))


def norm_kernel(most, y_ref, sq_ref, other_ref, empty_ref, gain_ref, out_ref):
    inverse = 1.0 / jnp.sqrt((sq_ref[...] + other_ref[...]) / F + EPSILON)
    empty = empty_ref[...]
    gain = gain_ref[...]
    for k in range(y_ref.shape[0] // most):
        place = slice(k * most, (k + 1) * most)
        out_ref[place, :] = y_ref[place, :] * gain * inverse[:, k : k + 1] + empty[:, k : k + 1]


def place_kernel(most, got_ref, out_ref, starts_v, starts_s, sem):
    nodes = got_ref.shape[0]
    size = nodes * most
    flags = as_bf16(got_ref[...].reshape(size, LANES) < LIMIT)
    slot = iota((nodes, size), 1)
    first = iota((nodes, size), 0) * most
    member = as_bf16((slot >= first) & (slot < first + most))
    counts = mm(member, flags)
    earlier = as_bf16(iota((nodes, nodes), 1) < iota((nodes, nodes), 0))
    starts = mm(earlier, counts.astype(jnp.bfloat16))
    diagonal = jnp.where(iota((nodes, LANES), 0) == iota((nodes, LANES), 1), starts, 0.0)
    starts_v[...] = jnp.sum(diagonal, axis=0, keepdims=True).astype(jnp.int32)
    copy = pltpu.make_async_copy(starts_v, starts_s, sem)
    copy.start()
    out_ref[...] = jnp.zeros_like(out_ref)
    copy.wait()

    for k in range(nodes):
        block = got_ref[k]
        out_ref[pl.ds(starts_s[0, k], most), :] = jnp.where(block < LIMIT, block, 0.0)


VMEM = pl.BlockSpec(memory_space=pltpu.VMEM)
ANY = pl.BlockSpec(memory_space=pl.ANY)


def local(rows, row_mask, key_bucket, gain):
    size_rows, half = rows.shape
    nodes = lax.axis_size("tm")
    most = 3 * size_rows // (4 * nodes)
    chunks = size_rows // LANES
    slots = nodes * most
    f32, bf16, i16 = jnp.float32, jnp.bfloat16, jnp.int16
    tail, xcat, crow, cs, empty = pl.pallas_call(
        functools.partial(index_kernel, most),
        out_shape=(
            jax.ShapeDtypeStruct((WINDOW, half), f32),
            jax.ShapeDtypeStruct((size_rows, 2 * half), bf16),
            jax.ShapeDtypeStruct((chunks, 16, LANES), i16),
            jax.ShapeDtypeStruct((slots, LANES), i16),
            jax.ShapeDtypeStruct((most, LANES), f32),
        ),
        in_specs=[ANY, VMEM, VMEM],
        out_specs=(VMEM,) * 5,
        scratch_shapes=[
            pltpu.VMEM((size_rows, half), f32),
            pltpu.VMEM((nodes, size_rows), bf16),
            pltpu.VMEM((96, size_rows), bf16),
            pltpu.SemaphoreType.DMA,
        ],
        name="index",
    )(rows, row_mask.reshape(chunks, LANES), key_bucket.reshape(chunks, LANES))
    earlier_tail = lax.ppermute(tail, "tm", [(i, (i + 1) % nodes) for i in range(nodes)])
    block = 384
    sums = pl.pallas_call(
        functools.partial(own_kernel, block),
        out_shape=jax.ShapeDtypeStruct((slots, half), f32),
        in_specs=[VMEM] * 3,
        out_specs=VMEM,
        scratch_shapes=[pltpu.VMEM((block, size_rows), bf16)],
        cost_estimate=pl.CostEstimate(flops=2 * slots * size_rows * 2 * half, bytes_accessed=4 * slots * half, transcendentals=0),
        name="own",
    )(xcat, crow, cs)
    y, sq = pl.pallas_call(
        functools.partial(tail_kernel, most),
        out_shape=(jax.ShapeDtypeStruct((slots, half), f32), jax.ShapeDtypeStruct((most, LANES), f32)),
        in_specs=[VMEM] * 3,
        out_specs=(VMEM,) * 2,
        name="tail",
    )(sums, earlier_tail, cs)
    other = lax.ppermute(sq, "rep", [(0, 1), (1, 0)])
    outgoing = pl.pallas_call(
        functools.partial(norm_kernel, most),
        out_shape=jax.ShapeDtypeStruct((slots, half), f32),
        in_specs=[VMEM] * 5,
        out_specs=VMEM,
        name="norm",
    )(y, sq, other, empty, gain.reshape(1, half))
    got = lax.all_to_all(outgoing.reshape(nodes, most * half), "tm", split_axis=0, concat_axis=0, tiled=True)
    got = got.reshape(nodes, most, half)
    return pl.pallas_call(
        functools.partial(place_kernel, most),
        out_shape=jax.ShapeDtypeStruct((slots, half), f32),
        in_specs=[VMEM],
        out_specs=VMEM,
        scratch_shapes=[pltpu.VMEM((1, LANES), jnp.int32), pltpu.SMEM((1, LANES), jnp.int32), pltpu.SemaphoreType.DMA],
        name="place",
    )(got)


def solution(mesh):
    in_specs = (P("tm", "rep"), P("tm"), P("tm"), P("rep"))
    out_specs = P("tm", "rep")
    return jax.shard_map(local, mesh=mesh, in_specs=in_specs, out_specs=out_specs, check_vma=False)
```

```python
import functools

import jax
import jax.numpy as jnp
from jax import lax
from jax.experimental import pallas as pl
from jax.experimental.pallas import tpu as pltpu
from jax.sharding import PartitionSpec as P

F = 256
WINDOW = 512
LANES = 128
EPSILON = 1e-06

BIAS = 32768
INSIDE = WINDOW - BIAS
NOT_LIVE = 16384
EMPTY_SLOT = 16384
EMPTY = 1e9
LIMIT = 1e8


def iota(shape, dim):
    return lax.broadcasted_iota(jnp.int32, shape, dim)


def as_bf16(test):
    return jnp.where(test, jnp.float32(1.0), jnp.float32(0.0)).astype(jnp.bfloat16)


def ones_where(test):
    return jnp.where(test, jnp.bfloat16(1.0), jnp.bfloat16(0.0))


def mm(a, b):
    return jnp.dot(a, b, preferred_element_type=jnp.float32)


def index_kernel(rows_ref, mask_ref, tail_ref, xcat_ref, crow_ref, c_ref, x_ref, m_ref, sems):
    size_rows = rows_ref.shape[0]
    chunks = size_rows // LANES
    load_mask = pltpu.make_async_copy(mask_ref, m_ref, sems.at[0])
    load_rows = pltpu.make_async_copy(rows_ref, x_ref, sems.at[1])
    load_mask.start()
    load_rows.start()
    load_mask.wait()
    mask = m_ref[...]
    mask_bf = mask.astype(jnp.float32).astype(jnp.bfloat16)
    upper = as_bf16(iota((LANES, LANES), 0) <= iota((LANES, LANES), 1))
    within = mm(mask_bf, upper)
    totals = mm(mask_bf, jnp.ones((LANES, LANES), jnp.bfloat16))
    below = as_bf16(iota((chunks, chunks), 1) < iota((chunks, chunks), 0))
    before = mm(below, totals.astype(jnp.bfloat16))
    count = (before + totals)[chunks - 1 : chunks, :].astype(jnp.int32)
    c = jnp.where(mask == 1, (within + before - 1.0).astype(jnp.int32), NOT_LIVE)
    c_ref[...] = c
    rows16 = [jnp.broadcast_to(c[a : a + 1, :], (16, LANES)).astype(jnp.int16) for a in range(chunks)]
    for a in range(chunks):
        crow_ref[a] = rows16[a]
    load_rows.wait()
    x = x_ref[...]
    high = x.astype(jnp.bfloat16)
    xcat_ref[:, :LANES] = high
    xcat_ref[:, LANES:] = (x - high.astype(jnp.float32)).astype(jnp.bfloat16)
    wanted = jnp.broadcast_to(count - WINDOW, (WINDOW, LANES)) + iota((WINDOW, LANES), 0)
    wanted = wanted.astype(jnp.int16)
    first = (size_rows // 2 - WINDOW) // LANES
    parts = []
    for a in range(first, chunks):
        parts.append(ones_where(wanted == jnp.broadcast_to(rows16[a][None], (WINDOW // 16, 16, LANES)).reshape(WINDOW, LANES)))
    both = mm(jnp.concatenate(parts, axis=1), xcat_ref[first * LANES :, :])
    tail_ref[...] = both[:, :LANES] + both[:, LANES:]


def find_slots(most, c_ref, key_ref, cs_ref, empty_ref, hits_ref, picks_ref):
    chunks = c_ref.shape[0]
    c = c_ref[...]
    key = jnp.where(c < NOT_LIVE, key_ref[...], -1)
    buckets = iota((LANES, LANES), 0)
    for a in range(chunks):
        hits_ref[:, a * LANES : (a + 1) * LANES] = as_bf16(jnp.broadcast_to(key[a : a + 1, :], (LANES, LANES)) == buckets)
    upper = as_bf16(iota((256, 256), 0) <= iota((256, 256), 1))
    carry = jnp.zeros((LANES, 1), jnp.float32)
    ranks = iota((32, LANES), 0)
    for b in range(chunks // 2):
        hits = hits_ref[:, b * 256 : (b + 1) * 256]
        running = mm(hits, upper)
        rank = jnp.sum(hits.astype(jnp.float32) * (running + carry), axis=0, keepdims=True) - 1.0
        carry = carry + running[:, 255:256]
        for h in range(2):
            a = 2 * b + h
            same = jnp.broadcast_to(rank[:, h * LANES : (h + 1) * LANES], (32, LANES)).astype(jnp.int32) == ranks
            high = jnp.broadcast_to((c[a : a + 1, :] >> 6).astype(jnp.float32), (32, LANES))
            low = jnp.broadcast_to((c[a : a + 1, :] & 63).astype(jnp.float32), (32, LANES))
            place = slice(a * LANES, (a + 1) * LANES)
            picks_ref[0:32, place] = jnp.where(same, high, 0.0).astype(jnp.bfloat16)
            picks_ref[32:64, place] = jnp.where(same, low, 0.0).astype(jnp.bfloat16)
            picks_ref[64:96, place] = jnp.where(same, 1.0, 0.0).astype(jnp.bfloat16)
    found = lax.dot_general(picks_ref[...], hits_ref[...], (((1,), (1,)), ((), ())), preferred_element_type=jnp.float32)
    filled = found[64:96, :] > 0.5
    slots = found[0:32, :] * 64.0 + found[32:64, :]
    slots = jnp.where(filled, slots.astype(jnp.int32) - BIAS, EMPTY_SLOT)
    empty_ref[...] = jnp.where(filled, 0.0, EMPTY)[:most, :]
    for k in range(0, LANES, 2):
        pair = [jnp.broadcast_to(slots[:most, k + j : k + j + 1], (most, LANES)) for j in range(2)]
        cs_ref[k * most : (k + 2) * most, :] = jnp.concatenate(pair, axis=0).astype(jnp.int16)


def own_kernel(most, block, xcat_ref, crow_ref, c_ref, key_ref, sums_ref, cs_ref, empty_ref, hits_ref, picks_ref):
    chunks = crow_ref.shape[0]
    find_slots(most, c_ref, key_ref, cs_ref, empty_ref, hits_ref, picks_ref)

    def step(m, carry):
        base = pl.multiple_of(m * block, block)
        cs = cs_ref[pl.ds(base, block), :]
        both = None
        for a in range(0, chunks, 2):
            parts = []
            for i in range(2):
                row = jnp.broadcast_to(crow_ref[a + i][None], (block // 16, 16, LANES)).reshape(block, LANES)
                parts.append(ones_where(cs - row < INSIDE))
            part = mm(jnp.concatenate(parts, axis=1), xcat_ref[a * LANES : (a + 2) * LANES, :])
            both = part if both is None else both + part
        sums_ref[pl.ds(base, block), :] = both[:, :LANES] + both[:, LANES:]
        return carry

    lax.fori_loop(0, cs_ref.shape[0] // block, step, 0)


def tail_kernel(most, sums_ref, tail_ref, cs_ref, y_ref, sq_ref):
    tail = tail_ref[...]
    high = tail.astype(jnp.bfloat16)
    tailcat = jnp.concatenate([high, (tail - high.astype(jnp.float32)).astype(jnp.bfloat16)], axis=1)
    lanes = iota((most, LANES), 1)
    group = 32
    size = group * most

    def add_tail(j, sq):
        base = pl.multiple_of(j * size, size)
        cs = cs_ref[pl.ds(base, size), :]
        parts = [
            ones_where(cs - (iota((size, LANES), 1) + (a * LANES - WINDOW)).astype(jnp.int16) < INSIDE) for a in range(WINDOW // LANES)
        ]
        both = mm(jnp.concatenate(parts, axis=1), tailcat)
        y = sums_ref[pl.ds(base, size), :] + both[:, :LANES] + both[:, LANES:]
        y_ref[pl.ds(base, size), :] = y
        squares = jnp.sum(y * y, axis=1, keepdims=True)
        for i in range(group):
            sq = jnp.where(lanes == j * group + i, squares[i * most : (i + 1) * most, :], sq)
        return sq

    sq_ref[...] = lax.fori_loop(0, y_ref.shape[0] // size, add_tail, jnp.zeros((most, LANES), jnp.float32))


def norm_kernel(y_ref, sq_ref, other_ref, empty_ref, gain_ref, out_ref):
    inverse = 1.0 / jnp.sqrt((sq_ref[...] + other_ref[...]) / F + EPSILON)
    empty = empty_ref[...]
    gain = gain_ref[...]
    for k in range(y_ref.shape[0]):
        out_ref[k] = y_ref[k] * gain * inverse[:, k : k + 1] + empty[:, k : k + 1]


def place_kernel(most, got_ref, out_ref, starts_v, starts_s, sem):
    nodes = got_ref.shape[0]
    size = nodes * most
    flags = as_bf16(got_ref[...].reshape(size, LANES) < LIMIT)
    slot = iota((nodes, size), 1)
    first = iota((nodes, size), 0) * most
    member = as_bf16((slot >= first) & (slot < first + most))
    counts = mm(member, flags)
    earlier = as_bf16(iota((nodes, nodes), 1) < iota((nodes, nodes), 0))
    starts = mm(earlier, counts.astype(jnp.bfloat16))
    diagonal = jnp.where(iota((nodes, LANES), 0) == iota((nodes, LANES), 1), starts, 0.0)
    starts_v[...] = jnp.sum(diagonal, axis=0, keepdims=True).astype(jnp.int32)
    copy = pltpu.make_async_copy(starts_v, starts_s, sem)
    copy.start()
    out_ref[...] = jnp.zeros_like(out_ref)
    copy.wait()

    for k in range(nodes):
        block = got_ref[k]
        out_ref[pl.ds(starts_s[0, k], most), :] = jnp.where(block < LIMIT, block, 0.0)


VMEM = pl.BlockSpec(memory_space=pltpu.VMEM)
HBM = pl.BlockSpec(memory_space=pltpu.HBM)


def call(kernel, name, outs, ins, scratch, megabytes, **settings):
    params = {"vmem_limit_bytes": megabytes << 20, **settings.pop("params", {})}
    return pl.pallas_call(
        kernel,
        out_shape=outs,
        in_specs=ins,
        out_specs=jax.tree.map(lambda _: VMEM, outs),
        scratch_shapes=scratch,
        compiler_params=pltpu.CompilerParams(**params),
        name=name,
        **settings,
    )


def local(rows, row_mask, key_bucket, gain):
    size_rows, half = rows.shape
    nodes = lax.axis_size("tm")
    most = 3 * size_rows // (4 * nodes)
    chunks = size_rows // LANES
    slots = nodes * most
    f32, bf16, i16, i32 = jnp.float32, jnp.bfloat16, jnp.int16, jnp.int32
    shape = jax.ShapeDtypeStruct
    dma = pltpu.SemaphoreType.DMA
    tail, xcat, crow, c = call(
        index_kernel,
        "index",
        (
            shape((WINDOW, half), f32),
            shape((size_rows, 2 * half), bf16),
            shape((chunks, 16, LANES), i16),
            shape((chunks, LANES), i32),
        ),
        [HBM, HBM],
        [pltpu.VMEM((size_rows, half), f32), pltpu.VMEM((chunks, LANES), i32), dma((2,))],
        50,
    )(rows, row_mask.reshape(chunks, LANES))
    earlier_tail = lax.ppermute(tail, "tm", [(i, (i + 1) % nodes) for i in range(nodes)])
    sums, cs, empty = call(
        functools.partial(own_kernel, most, 32 * most),
        "own",
        (shape((slots, half), f32), shape((slots, LANES), i16), shape((most, LANES), f32)),
        [VMEM] * 4,
        [
            pltpu.VMEM((nodes, size_rows), bf16),
            pltpu.VMEM((96, size_rows), bf16),
        ],
        24,
        cost_estimate=pl.CostEstimate(flops=2 * slots * size_rows * 2 * half, bytes_accessed=4 * slots * half, transcendentals=0),
    )(xcat, crow, c, key_bucket.reshape(chunks, LANES))
    y, sq = call(
        functools.partial(tail_kernel, most),
        "tail",
        (shape((slots, half), f32), shape((most, LANES), f32)),
        [VMEM] * 3,
        [],
        20,
    )(sums, earlier_tail, cs)
    other = lax.ppermute(sq, "rep", [(0, 1), (1, 0)])
    outgoing = call(
        norm_kernel,
        "norm",
        shape((nodes, most, half), f32),
        [VMEM] * 5,
        [],
        12,
    )(y.reshape(nodes, most, half), sq, other, empty, gain.reshape(1, half))
    got = lax.all_to_all(outgoing.reshape(nodes, most * half), "tm", split_axis=0, concat_axis=0, tiled=True)
    got = got.reshape(nodes, most, half)
    return call(
        functools.partial(place_kernel, most),
        "place",
        shape((slots, half), f32),
        [VMEM],
        [pltpu.VMEM((1, LANES), i32), pltpu.SMEM((1, LANES), i32), dma],
        20,
    )(got)


def solution(mesh):
    in_specs = (P("tm", "rep"), P("tm"), P("tm"), P("rep"))
    out_specs = P("tm", "rep")
    return jax.shard_map(local, mesh=mesh, in_specs=in_specs, out_specs=out_specs, check_vma=False)
```

```python
import functools

import jax
import jax.numpy as jnp
from jax import lax
from jax.experimental import pallas as pl
from jax.experimental.pallas import tpu as pltpu
from jax.sharding import PartitionSpec as P

F = 256
WINDOW = 512
LANES = 128
EPSILON = 1e-06
MESH = pl.DeviceIdType.MESH

BIAS = 32768
INSIDE = WINDOW - BIAS
NOT_LIVE = 16384
EMPTY_SLOT = 16384
EMPTY = 1e9
LIMIT = 1e8


def iota(shape, dim):
    return lax.broadcasted_iota(jnp.int32, shape, dim)


def as_bf16(test):
    return jnp.where(test, jnp.float32(1.0), jnp.float32(0.0)).astype(jnp.bfloat16)


def ones_where(test):
    return jnp.where(test, jnp.bfloat16(1.0), jnp.bfloat16(0.0))


def mm(a, b):
    return jnp.dot(a, b, preferred_element_type=jnp.float32)


def index_kernel(rows_ref, mask_ref, tail_ref, xcat_ref, crow_ref, c_ref, x_ref, m_ref, sems):
    size_rows = rows_ref.shape[0]
    chunks = size_rows // LANES
    load_mask = pltpu.make_async_copy(mask_ref, m_ref, sems.at[0])
    load_rows = pltpu.make_async_copy(rows_ref, x_ref, sems.at[1])
    load_mask.start()
    load_rows.start()
    load_mask.wait()
    mask = m_ref[...]
    mask_bf = mask.astype(jnp.float32).astype(jnp.bfloat16)
    upper = as_bf16(iota((LANES, LANES), 0) <= iota((LANES, LANES), 1))
    within = mm(mask_bf, upper)
    totals = mm(mask_bf, jnp.ones((LANES, LANES), jnp.bfloat16))
    below = as_bf16(iota((chunks, chunks), 1) < iota((chunks, chunks), 0))
    before = mm(below, totals.astype(jnp.bfloat16))
    count = (before + totals)[chunks - 1 : chunks, :].astype(jnp.int32)
    c = jnp.where(mask == 1, (within + before - 1.0).astype(jnp.int32), NOT_LIVE)
    c_ref[...] = c
    rows16 = [jnp.broadcast_to(c[a : a + 1, :], (16, LANES)).astype(jnp.int16) for a in range(chunks)]
    for a in range(chunks):
        crow_ref[a] = rows16[a]
    load_rows.wait()
    x = x_ref[...]
    high = x.astype(jnp.bfloat16)
    xcat_ref[:, :LANES] = high
    xcat_ref[:, LANES:] = (x - high.astype(jnp.float32)).astype(jnp.bfloat16)
    wanted = jnp.broadcast_to(count - WINDOW, (WINDOW, LANES)) + iota((WINDOW, LANES), 0)
    wanted = wanted.astype(jnp.int16)
    first = (size_rows // 2 - WINDOW) // LANES
    parts = []
    for a in range(first, chunks):
        parts.append(ones_where(wanted == jnp.broadcast_to(rows16[a][None], (WINDOW // 16, 16, LANES)).reshape(WINDOW, LANES)))
    both = mm(jnp.concatenate(parts, axis=1), xcat_ref[first * LANES :, :])
    tail_ref[...] = both[:, :LANES] + both[:, LANES:]


def find_slots(most, c_ref, key_ref, cs_ref, empty_ref, hits_ref, picks_ref):
    chunks = c_ref.shape[0]
    c = c_ref[...]
    key = jnp.where(c < NOT_LIVE, key_ref[...], -1)
    buckets = iota((LANES, LANES), 0)
    for a in range(chunks):
        hits_ref[:, a * LANES : (a + 1) * LANES] = as_bf16(jnp.broadcast_to(key[a : a + 1, :], (LANES, LANES)) == buckets)
    upper = as_bf16(iota((256, 256), 0) <= iota((256, 256), 1))
    carry = jnp.zeros((LANES, 1), jnp.float32)
    ranks = iota((32, LANES), 0)
    for b in range(chunks // 2):
        hits = hits_ref[:, b * 256 : (b + 1) * 256]
        running = mm(hits, upper)
        rank = jnp.sum(hits.astype(jnp.float32) * (running + carry), axis=0, keepdims=True) - 1.0
        carry = carry + running[:, 255:256]
        for h in range(2):
            a = 2 * b + h
            same = jnp.broadcast_to(rank[:, h * LANES : (h + 1) * LANES], (32, LANES)).astype(jnp.int32) == ranks
            high = jnp.broadcast_to((c[a : a + 1, :] >> 6).astype(jnp.float32), (32, LANES))
            low = jnp.broadcast_to((c[a : a + 1, :] & 63).astype(jnp.float32), (32, LANES))
            place = slice(a * LANES, (a + 1) * LANES)
            picks_ref[0:32, place] = jnp.where(same, high, 0.0).astype(jnp.bfloat16)
            picks_ref[32:64, place] = jnp.where(same, low, 0.0).astype(jnp.bfloat16)
            picks_ref[64:96, place] = jnp.where(same, 1.0, 0.0).astype(jnp.bfloat16)
    found = lax.dot_general(picks_ref[...], hits_ref[...], (((1,), (1,)), ((), ())), preferred_element_type=jnp.float32)
    filled = found[64:96, :] > 0.5
    slots = found[0:32, :] * 64.0 + found[32:64, :]
    slots = jnp.where(filled, slots.astype(jnp.int32) - BIAS, EMPTY_SLOT)
    empty_ref[...] = jnp.where(filled, 0.0, EMPTY)[:most, :]
    for k in range(0, LANES, 2):
        pair = [jnp.broadcast_to(slots[:most, k + j : k + j + 1], (most, LANES)) for j in range(2)]
        cs_ref[k * most : (k + 2) * most, :] = jnp.concatenate(pair, axis=0).astype(jnp.int16)


def own_kernel(most, block, xcat_ref, crow_ref, c_ref, key_ref, sums_ref, cs_ref, empty_ref, hits_ref, picks_ref):
    chunks = crow_ref.shape[0]
    find_slots(most, c_ref, key_ref, cs_ref, empty_ref, hits_ref, picks_ref)

    def step(m, carry):
        base = pl.multiple_of(m * block, block)
        cs = cs_ref[pl.ds(base, block), :]
        both = None
        for a in range(0, chunks, 2):
            parts = []
            for i in range(2):
                row = jnp.broadcast_to(crow_ref[a + i][None], (block // 16, 16, LANES)).reshape(block, LANES)
                parts.append(ones_where(cs - row < INSIDE))
            part = mm(jnp.concatenate(parts, axis=1), xcat_ref[a * LANES : (a + 2) * LANES, :])
            both = part if both is None else both + part
        sums_ref[pl.ds(base, block), :] = both[:, :LANES] + both[:, LANES:]
        return carry

    lax.fori_loop(0, cs_ref.shape[0] // block, step, 0)


def tail_kernel(most, sums_ref, tail_ref, cs_ref, y_ref, sq_ref):
    tail = tail_ref[...]
    high = tail.astype(jnp.bfloat16)
    tailcat = jnp.concatenate([high, (tail - high.astype(jnp.float32)).astype(jnp.bfloat16)], axis=1)
    lanes = iota((most, LANES), 1)
    group = 32
    size = group * most

    def add_tail(j, sq):
        base = pl.multiple_of(j * size, size)
        cs = cs_ref[pl.ds(base, size), :]
        parts = [
            ones_where(cs - (iota((size, LANES), 1) + (a * LANES - WINDOW)).astype(jnp.int16) < INSIDE) for a in range(WINDOW // LANES)
        ]
        both = mm(jnp.concatenate(parts, axis=1), tailcat)
        y = sums_ref[pl.ds(base, size), :] + both[:, :LANES] + both[:, LANES:]
        y_ref[pl.ds(base, size), :] = y
        squares = jnp.sum(y * y, axis=1, keepdims=True)
        for i in range(group):
            sq = jnp.where(lanes == j * group + i, squares[i * most : (i + 1) * most, :], sq)
        return sq

    sq_ref[...] = lax.fori_loop(0, y_ref.shape[0] // size, add_tail, jnp.zeros((most, LANES), jnp.float32))


def norm_kernel(y_ref, sq_ref, other_ref, empty_ref, gain_ref, out_ref):
    inverse = 1.0 / jnp.sqrt((sq_ref[...] + other_ref[...]) / F + EPSILON)
    empty = empty_ref[...]
    gain = gain_ref[...]
    for k in range(y_ref.shape[0]):
        out_ref[k] = y_ref[k] * gain * inverse[:, k : k + 1] + empty[:, k : k + 1]


def exchange_kernel(nodes, out_ref, got_ref, send_sem, recv_sem):
    me, rep = lax.axis_index("tm"), lax.axis_index("rep")
    barrier = pltpu.get_barrier_semaphore()

    def greet(k, carry):
        pl.semaphore_signal(barrier, inc=1, device_id=(lax.rem(me + k, nodes), rep), device_id_type=MESH)
        return carry

    lax.fori_loop(1, nodes, greet, 0)
    got_ref[me] = out_ref[me]
    pl.semaphore_wait(barrier, nodes - 1)

    def send(k, carry):
        to = lax.rem(me + k, nodes)
        pltpu.make_async_remote_copy(
            src_ref=out_ref.at[to],
            dst_ref=got_ref.at[me],
            send_sem=send_sem,
            recv_sem=recv_sem,
            device_id=(to, rep),
            device_id_type=MESH,
        ).start()
        return carry

    lax.fori_loop(1, nodes, send, 0)
    others = pl.ds(0, nodes - 1)
    every = pltpu.make_async_remote_copy(
        src_ref=out_ref.at[others],
        dst_ref=got_ref.at[others],
        send_sem=send_sem,
        recv_sem=recv_sem,
        device_id=(me, 1 - rep),
        device_id_type=MESH,
    )
    every.wait_send()
    every.wait_recv()


def place_kernel(most, got_ref, out_ref, starts_v, starts_s, sem):
    nodes = got_ref.shape[0]
    size = nodes * most
    flags = as_bf16(got_ref[...].reshape(size, LANES) < LIMIT)
    slot = iota((nodes, size), 1)
    first = iota((nodes, size), 0) * most
    member = as_bf16((slot >= first) & (slot < first + most))
    counts = mm(member, flags)
    earlier = as_bf16(iota((nodes, nodes), 1) < iota((nodes, nodes), 0))
    starts = mm(earlier, counts.astype(jnp.bfloat16))
    diagonal = jnp.where(iota((nodes, LANES), 0) == iota((nodes, LANES), 1), starts, 0.0)
    starts_v[...] = jnp.sum(diagonal, axis=0, keepdims=True).astype(jnp.int32)
    copy = pltpu.make_async_copy(starts_v, starts_s, sem)
    copy.start()
    out_ref[...] = jnp.zeros_like(out_ref)
    copy.wait()

    for k in range(nodes):
        block = got_ref[k]
        out_ref[pl.ds(starts_s[0, k], most), :] = jnp.where(block < LIMIT, block, 0.0)


VMEM = pl.BlockSpec(memory_space=pltpu.VMEM)
HBM = pl.BlockSpec(memory_space=pltpu.HBM)


def call(kernel, name, outs, ins, scratch, megabytes, **settings):
    params = {"vmem_limit_bytes": megabytes << 20, **settings.pop("params", {})}
    return pl.pallas_call(
        kernel,
        out_shape=outs,
        in_specs=ins,
        out_specs=jax.tree.map(lambda _: VMEM, outs),
        scratch_shapes=scratch,
        compiler_params=pltpu.CompilerParams(**params),
        name=name,
        **settings,
    )


def local(rows, row_mask, key_bucket, gain):
    size_rows, half = rows.shape
    nodes = lax.axis_size("tm")
    most = 3 * size_rows // (4 * nodes)
    chunks = size_rows // LANES
    slots = nodes * most
    f32, bf16, i16, i32 = jnp.float32, jnp.bfloat16, jnp.int16, jnp.int32
    shape = jax.ShapeDtypeStruct
    dma = pltpu.SemaphoreType.DMA
    tail, xcat, crow, c = call(
        index_kernel,
        "index",
        (
            shape((WINDOW, half), f32),
            shape((size_rows, 2 * half), bf16),
            shape((chunks, 16, LANES), i16),
            shape((chunks, LANES), i32),
        ),
        [HBM, HBM],
        [pltpu.VMEM((size_rows, half), f32), pltpu.VMEM((chunks, LANES), i32), dma((2,))],
        50,
    )(rows, row_mask.reshape(chunks, LANES))
    earlier_tail = lax.ppermute(tail, "tm", [(i, (i + 1) % nodes) for i in range(nodes)])
    sums, cs, empty = call(
        functools.partial(own_kernel, most, 32 * most),
        "own",
        (shape((slots, half), f32), shape((slots, LANES), i16), shape((most, LANES), f32)),
        [VMEM] * 4,
        [
            pltpu.VMEM((nodes, size_rows), bf16),
            pltpu.VMEM((96, size_rows), bf16),
        ],
        24,
        cost_estimate=pl.CostEstimate(flops=2 * slots * size_rows * 2 * half, bytes_accessed=4 * slots * half, transcendentals=0),
    )(xcat, crow, c, key_bucket.reshape(chunks, LANES))
    y, sq = call(
        functools.partial(tail_kernel, most),
        "tail",
        (shape((slots, half), f32), shape((most, LANES), f32)),
        [VMEM] * 3,
        [],
        20,
    )(sums, earlier_tail, cs)
    other = lax.ppermute(sq, "rep", [(0, 1), (1, 0)])
    outgoing = call(
        norm_kernel,
        "norm",
        shape((nodes, most, half), f32),
        [VMEM] * 5,
        [],
        12,
    )(y.reshape(nodes, most, half), sq, other, empty, gain.reshape(1, half))
    got = call(
        functools.partial(exchange_kernel, nodes),
        "exchange",
        shape((nodes, most, half), f32),
        [VMEM],
        [dma, dma],
        12,
        params={"collective_id": 0, "has_side_effects": True},
    )(outgoing)
    return call(
        functools.partial(place_kernel, most),
        "place",
        shape((slots, half), f32),
        [VMEM],
        [pltpu.VMEM((1, LANES), i32), pltpu.SMEM((1, LANES), i32), dma],
        20,
    )(got)


def solution(mesh):
    in_specs = (P("tm", "rep"), P("tm"), P("tm"), P("rep"))
    out_specs = P("tm", "rep")
    return jax.shard_map(local, mesh=mesh, in_specs=in_specs, out_specs=out_specs, check_vma=False)
```

```python
import functools

import jax
import jax.numpy as jnp
from jax import lax
from jax.experimental import pallas as pl
from jax.experimental.pallas import tpu as pltpu
from jax.sharding import PartitionSpec as P

F = 256
WINDOW = 512
LANES = 128
EPSILON = 1e-06
MESH = pl.DeviceIdType.MESH

BIAS = 32768
INSIDE = WINDOW - BIAS
NOT_LIVE = 16384
EMPTY_SLOT = 16384
EMPTY = 1e9
LIMIT = 1e8


def iota(shape, dim):
    return lax.broadcasted_iota(jnp.int32, shape, dim)


def as_bf16(test):
    return jnp.where(test, jnp.float32(1.0), jnp.float32(0.0)).astype(jnp.bfloat16)


def ones_where(test):
    return jnp.where(test, jnp.bfloat16(1.0), jnp.bfloat16(0.0))


def mm(a, b):
    return jnp.dot(a, b, preferred_element_type=jnp.float32)


def index_kernel(rows_ref, mask_ref, tail_ref, xcat_ref, crow_ref, c_ref, x_ref, m_ref, sems):
    size_rows = rows_ref.shape[0]
    chunks = size_rows // LANES
    load_mask = pltpu.make_async_copy(mask_ref, m_ref, sems.at[0])
    load_rows = pltpu.make_async_copy(rows_ref, x_ref, sems.at[1])
    load_mask.start()
    load_rows.start()
    load_mask.wait()
    mask = m_ref[...]
    mask_bf = mask.astype(jnp.float32).astype(jnp.bfloat16)
    upper = as_bf16(iota((LANES, LANES), 0) <= iota((LANES, LANES), 1))
    within = mm(mask_bf, upper)
    totals = mm(mask_bf, jnp.ones((LANES, LANES), jnp.bfloat16))
    below = as_bf16(iota((chunks, chunks), 1) < iota((chunks, chunks), 0))
    before = mm(below, totals.astype(jnp.bfloat16))
    count = (before + totals)[chunks - 1 : chunks, :].astype(jnp.int32)
    c = jnp.where(mask == 1, (within + before - 1.0).astype(jnp.int32), NOT_LIVE)
    c_ref[...] = c
    rows16 = [jnp.broadcast_to(c[a : a + 1, :], (16, LANES)).astype(jnp.int16) for a in range(chunks)]
    for a in range(chunks):
        crow_ref[a] = rows16[a]
    load_rows.wait()
    x = x_ref[...]
    high = x.astype(jnp.bfloat16)
    xcat_ref[:, :LANES] = high
    xcat_ref[:, LANES:] = (x - high.astype(jnp.float32)).astype(jnp.bfloat16)
    wanted = jnp.broadcast_to(count - WINDOW, (WINDOW, LANES)) + iota((WINDOW, LANES), 0)
    wanted = wanted.astype(jnp.int16)
    first = (size_rows // 2 - WINDOW) // LANES
    parts = []
    for a in range(first, chunks):
        parts.append(ones_where(wanted == jnp.broadcast_to(rows16[a][None], (WINDOW // 16, 16, LANES)).reshape(WINDOW, LANES)))
    both = mm(jnp.concatenate(parts, axis=1), xcat_ref[first * LANES :, :])
    tail_ref[...] = both[:, :LANES] + both[:, LANES:]


def find_slots(most, c_ref, key_ref, cs_ref, empty_ref, hits_ref, picks_ref):
    chunks = c_ref.shape[0]
    c = c_ref[...]
    key = jnp.where(c < NOT_LIVE, key_ref[...], -1)
    buckets = iota((LANES, LANES), 0)
    for a in range(chunks):
        hits_ref[:, a * LANES : (a + 1) * LANES] = as_bf16(jnp.broadcast_to(key[a : a + 1, :], (LANES, LANES)) == buckets)
    upper = as_bf16(iota((256, 256), 0) <= iota((256, 256), 1))
    carry = jnp.zeros((LANES, 1), jnp.float32)
    ranks = iota((32, LANES), 0)
    for b in range(chunks // 2):
        hits = hits_ref[:, b * 256 : (b + 1) * 256]
        running = mm(hits, upper)
        rank = jnp.sum(hits.astype(jnp.float32) * (running + carry), axis=0, keepdims=True) - 1.0
        carry = carry + running[:, 255:256]
        for h in range(2):
            a = 2 * b + h
            same = jnp.broadcast_to(rank[:, h * LANES : (h + 1) * LANES], (32, LANES)).astype(jnp.int32) == ranks
            high = jnp.broadcast_to((c[a : a + 1, :] >> 6).astype(jnp.float32), (32, LANES))
            low = jnp.broadcast_to((c[a : a + 1, :] & 63).astype(jnp.float32), (32, LANES))
            place = slice(a * LANES, (a + 1) * LANES)
            picks_ref[0:32, place] = jnp.where(same, high, 0.0).astype(jnp.bfloat16)
            picks_ref[32:64, place] = jnp.where(same, low, 0.0).astype(jnp.bfloat16)
            picks_ref[64:96, place] = jnp.where(same, 1.0, 0.0).astype(jnp.bfloat16)
    found = lax.dot_general(picks_ref[...], hits_ref[...], (((1,), (1,)), ((), ())), preferred_element_type=jnp.float32)
    filled = found[64:96, :] > 0.5
    slots = found[0:32, :] * 64.0 + found[32:64, :]
    slots = jnp.where(filled, slots.astype(jnp.int32) - BIAS, EMPTY_SLOT)
    empty_ref[...] = jnp.where(filled, 0.0, EMPTY)[:most, :]
    for k in range(0, LANES, 2):
        pair = [jnp.broadcast_to(slots[:most, k + j : k + j + 1], (most, LANES)) for j in range(2)]
        cs_ref[k * most : (k + 2) * most, :] = jnp.concatenate(pair, axis=0).astype(jnp.int16)


def own_kernel(most, block, xcat_ref, crow_ref, c_ref, key_ref, sums_ref, cs_ref, empty_ref, hits_ref, picks_ref):
    chunks = crow_ref.shape[0]
    find_slots(most, c_ref, key_ref, cs_ref, empty_ref, hits_ref, picks_ref)

    def step(m, carry):
        base = pl.multiple_of(m * block, block)
        cs = cs_ref[pl.ds(base, block), :]
        both = None
        for a in range(0, chunks, 2):
            parts = []
            for i in range(2):
                row = jnp.broadcast_to(crow_ref[a + i][None], (block // 16, 16, LANES)).reshape(block, LANES)
                parts.append(ones_where(cs - row < INSIDE))
            part = mm(jnp.concatenate(parts, axis=1), xcat_ref[a * LANES : (a + 2) * LANES, :])
            both = part if both is None else both + part
        sums_ref[pl.ds(base, block), :] = both[:, :LANES] + both[:, LANES:]
        return carry

    lax.fori_loop(0, cs_ref.shape[0] // block, step, 0)


def tail_kernel(most, sums_ref, tail_ref, cs_ref, y_ref, sq_ref):
    tail = tail_ref[...]
    high = tail.astype(jnp.bfloat16)
    tailcat = jnp.concatenate([high, (tail - high.astype(jnp.float32)).astype(jnp.bfloat16)], axis=1)
    lanes = iota((most, LANES), 1)
    group = 32
    size = group * most

    def add_tail(j, sq):
        base = pl.multiple_of(j * size, size)
        cs = cs_ref[pl.ds(base, size), :]
        parts = [
            ones_where(cs - (iota((size, LANES), 1) + (a * LANES - WINDOW)).astype(jnp.int16) < INSIDE) for a in range(WINDOW // LANES)
        ]
        both = mm(jnp.concatenate(parts, axis=1), tailcat)
        y = sums_ref[pl.ds(base, size), :] + both[:, :LANES] + both[:, LANES:]
        y_ref[pl.ds(base, size), :] = y
        squares = jnp.sum(y * y, axis=1, keepdims=True)
        for i in range(group):
            sq = jnp.where(lanes == j * group + i, squares[i * most : (i + 1) * most, :], sq)
        return sq

    sq_ref[...] = lax.fori_loop(0, y_ref.shape[0] // size, add_tail, jnp.zeros((most, LANES), jnp.float32))


def exchange_kernel(nodes, most, y_ref, sq_ref, other_ref, empty_ref, gain_ref, got_ref, out_ref, send_sem, recv_sem):
    me, rep = lax.axis_index("tm"), lax.axis_index("rep")
    barrier = pltpu.get_barrier_semaphore()

    def greet(k, carry):
        pl.semaphore_signal(barrier, inc=1, device_id=(lax.rem(me + k, nodes), rep), device_id_type=MESH)
        return carry

    lax.fori_loop(1, nodes, greet, 0)
    inverse = 1.0 / jnp.sqrt((sq_ref[...] + other_ref[...]) / F + EPSILON)
    empty = empty_ref[...]
    gain = gain_ref[...]
    for k in range(nodes):
        out_ref[k] = y_ref[k] * gain * inverse[:, k : k + 1] + empty[:, k : k + 1]
    got_ref[me] = out_ref[me]
    pl.semaphore_wait(barrier, nodes - 1)

    def send(k, carry):
        to = lax.rem(me + k, nodes)
        pltpu.make_async_remote_copy(
            src_ref=out_ref.at[to],
            dst_ref=got_ref.at[me],
            send_sem=send_sem,
            recv_sem=recv_sem,
            device_id=(to, rep),
            device_id_type=MESH,
        ).start()
        return carry

    lax.fori_loop(1, nodes, send, 0)
    others = pl.ds(0, nodes - 1)
    every = pltpu.make_async_remote_copy(
        src_ref=out_ref.at[others],
        dst_ref=got_ref.at[others],
        send_sem=send_sem,
        recv_sem=recv_sem,
        device_id=(me, 1 - rep),
        device_id_type=MESH,
    )
    every.wait_send()
    every.wait_recv()


def place_kernel(most, got_ref, out_ref, starts_v, starts_s, sem):
    nodes = got_ref.shape[0]
    size = nodes * most
    flags = as_bf16(got_ref[...].reshape(size, LANES) < LIMIT)
    slot = iota((nodes, size), 1)
    first = iota((nodes, size), 0) * most
    member = as_bf16((slot >= first) & (slot < first + most))
    counts = mm(member, flags)
    earlier = as_bf16(iota((nodes, nodes), 1) < iota((nodes, nodes), 0))
    starts = mm(earlier, counts.astype(jnp.bfloat16))
    diagonal = jnp.where(iota((nodes, LANES), 0) == iota((nodes, LANES), 1), starts, 0.0)
    starts_v[...] = jnp.sum(diagonal, axis=0, keepdims=True).astype(jnp.int32)
    copy = pltpu.make_async_copy(starts_v, starts_s, sem)
    copy.start()
    out_ref[...] = jnp.zeros_like(out_ref)
    copy.wait()

    for k in range(nodes):
        block = got_ref[k]
        out_ref[pl.ds(starts_s[0, k], most), :] = jnp.where(block < LIMIT, block, 0.0)


VMEM = pl.BlockSpec(memory_space=pltpu.VMEM)
HBM = pl.BlockSpec(memory_space=pltpu.HBM)


def call(kernel, name, outs, ins, scratch, megabytes, **settings):
    params = {"vmem_limit_bytes": megabytes << 20, **settings.pop("params", {})}
    return pl.pallas_call(
        kernel,
        out_shape=outs,
        in_specs=ins,
        out_specs=jax.tree.map(lambda _: VMEM, outs),
        scratch_shapes=scratch,
        compiler_params=pltpu.CompilerParams(**params),
        name=name,
        **settings,
    )


def local(rows, row_mask, key_bucket, gain):
    size_rows, half = rows.shape
    nodes = lax.axis_size("tm")
    most = 3 * size_rows // (4 * nodes)
    chunks = size_rows // LANES
    slots = nodes * most
    f32, bf16, i16, i32 = jnp.float32, jnp.bfloat16, jnp.int16, jnp.int32
    shape = jax.ShapeDtypeStruct
    dma = pltpu.SemaphoreType.DMA
    tail, xcat, crow, c = call(
        index_kernel,
        "index",
        (
            shape((WINDOW, half), f32),
            shape((size_rows, 2 * half), bf16),
            shape((chunks, 16, LANES), i16),
            shape((chunks, LANES), i32),
        ),
        [HBM, HBM],
        [pltpu.VMEM((size_rows, half), f32), pltpu.VMEM((chunks, LANES), i32), dma((2,))],
        50,
    )(rows, pltpu.with_memory_space_constraint(row_mask.reshape(chunks, LANES), pltpu.HBM))
    earlier_tail = lax.ppermute(tail, "tm", [(i, (i + 1) % nodes) for i in range(nodes)])
    sums, cs, empty = call(
        functools.partial(own_kernel, most, 32 * most),
        "own",
        (shape((slots, half), f32), shape((slots, LANES), i16), shape((most, LANES), f32)),
        [VMEM] * 4,
        [
            pltpu.VMEM((nodes, size_rows), bf16),
            pltpu.VMEM((96, size_rows), bf16),
        ],
        24,
        cost_estimate=pl.CostEstimate(flops=2 * slots * size_rows * 2 * half, bytes_accessed=4 * slots * half, transcendentals=0),
    )(xcat, crow, c, key_bucket.reshape(chunks, LANES))
    y, sq = call(
        functools.partial(tail_kernel, most),
        "tail",
        (shape((slots, half), f32), shape((most, LANES), f32)),
        [VMEM] * 3,
        [],
        20,
    )(sums, earlier_tail, cs)
    other = lax.ppermute(sq, "rep", [(0, 1), (1, 0)])
    got = call(
        functools.partial(exchange_kernel, nodes, most),
        "exchange",
        shape((nodes, most, half), f32),
        [VMEM] * 5,
        [pltpu.VMEM((nodes, most, half), f32), dma, dma],
        12,
        params={"collective_id": 0, "has_side_effects": True},
    )(y.reshape(nodes, most, half), sq, other, empty, gain.reshape(1, half))
    return call(
        functools.partial(place_kernel, most),
        "place",
        shape((slots, half), f32),
        [VMEM],
        [pltpu.VMEM((1, LANES), i32), pltpu.SMEM((1, LANES), i32), dma],
        20,
    )(got)


def solution(mesh):
    in_specs = (P("tm", "rep"), P("tm"), P("tm"), P("rep"))
    out_specs = P("tm", "rep")
    return jax.shard_map(local, mesh=mesh, in_specs=in_specs, out_specs=out_specs, check_vma=False)
```

```python
import functools

import jax
import jax.numpy as jnp
from jax import lax
from jax.experimental import pallas as pl
from jax.experimental.pallas import tpu as pltpu
from jax.sharding import PartitionSpec as P

F = 256
WINDOW = 512
LANES = 128
EPSILON = 1e-06
MESH = pl.DeviceIdType.MESH

BIAS = 32768
INSIDE = WINDOW - BIAS
NOT_LIVE = 16384
EMPTY_SLOT = 16384
EMPTY = 1e9
LIMIT = 1e8


def iota(shape, dim):
    return lax.broadcasted_iota(jnp.int32, shape, dim)


def as_bf16(test):
    return jnp.where(test, jnp.float32(1.0), jnp.float32(0.0)).astype(jnp.bfloat16)


def ones_where(test):
    return jnp.where(test, jnp.bfloat16(1.0), jnp.bfloat16(0.0))


def mm(a, b):
    return jnp.dot(a, b, preferred_element_type=jnp.float32)


def find_tail(x, mask, tail_ref, xcat_ref, crow_ref, c_ref, wait_rows):
    size_rows = xcat_ref.shape[0]
    chunks = size_rows // LANES
    mask_bf = mask.astype(jnp.float32).astype(jnp.bfloat16)
    upper = as_bf16(iota((LANES, LANES), 0) <= iota((LANES, LANES), 1))
    within = mm(mask_bf, upper)
    totals = mm(mask_bf, jnp.ones((LANES, LANES), jnp.bfloat16))
    below = as_bf16(iota((chunks, chunks), 1) < iota((chunks, chunks), 0))
    before = mm(below, totals.astype(jnp.bfloat16))
    count = (before + totals)[chunks - 1 : chunks, :].astype(jnp.int32)
    c = jnp.where(mask == 1, (within + before - 1.0).astype(jnp.int32), NOT_LIVE)
    c_ref[...] = c
    rows16 = [jnp.broadcast_to(c[a : a + 1, :], (16, LANES)).astype(jnp.int16) for a in range(chunks)]
    for a in range(chunks):
        crow_ref[a] = rows16[a]
    wait_rows()
    high = x[...].astype(jnp.bfloat16)
    xcat_ref[:, :LANES] = high
    xcat_ref[:, LANES:] = (x[...] - high.astype(jnp.float32)).astype(jnp.bfloat16)
    wanted = jnp.broadcast_to(count - WINDOW, (WINDOW, LANES)) + iota((WINDOW, LANES), 0)
    wanted = wanted.astype(jnp.int16)
    first = (size_rows // 2 - WINDOW) // LANES
    parts = []
    for a in range(first, chunks):
        parts.append(ones_where(wanted == jnp.broadcast_to(rows16[a][None], (WINDOW // 16, 16, LANES)).reshape(WINDOW, LANES)))
    both = mm(jnp.concatenate(parts, axis=1), xcat_ref[first * LANES :, :])
    tail_ref[...] = both[:, :LANES] + both[:, LANES:]


def find_slots(most, group, c_ref, key_ref, cs_ref, empty_ref, hits_ref, picks_ref):
    chunks = c_ref.shape[0]
    c = c_ref[...]
    key = jnp.where(c < NOT_LIVE, key_ref[...], -1)
    buckets = iota((LANES, LANES), 0)
    for a in range(chunks):
        hits_ref[:, a * LANES : (a + 1) * LANES] = as_bf16(jnp.broadcast_to(key[a : a + 1, :], (LANES, LANES)) == buckets)
    upper = as_bf16(iota((256, 256), 0) <= iota((256, 256), 1))
    carry = jnp.zeros((LANES, 1), jnp.float32)
    ranks = iota((32, LANES), 0)
    for b in range(chunks // 2):
        hits = hits_ref[:, b * 256 : (b + 1) * 256]
        running = mm(hits, upper)
        rank = jnp.sum(hits.astype(jnp.float32) * (running + carry), axis=0, keepdims=True) - 1.0
        carry = carry + running[:, 255:256]
        for h in range(2):
            a = 2 * b + h
            same = jnp.broadcast_to(rank[:, h * LANES : (h + 1) * LANES], (32, LANES)).astype(jnp.int32) == ranks
            high = jnp.broadcast_to((c[a : a + 1, :] >> 6).astype(jnp.float32), (32, LANES))
            low = jnp.broadcast_to((c[a : a + 1, :] & 63).astype(jnp.float32), (32, LANES))
            place = slice(a * LANES, (a + 1) * LANES)
            picks_ref[0:32, place] = jnp.where(same, high, 0.0).astype(jnp.bfloat16)
            picks_ref[32:64, place] = jnp.where(same, low, 0.0).astype(jnp.bfloat16)
            picks_ref[64:96, place] = jnp.where(same, 1.0, 0.0).astype(jnp.bfloat16)
    found = lax.dot_general(picks_ref[...], hits_ref[...], (((1,), (1,)), ((), ())), preferred_element_type=jnp.float32)
    filled = found[64:96, :] > 0.5
    slots = found[0:32, :] * 64.0 + found[32:64, :]
    slots = jnp.where(filled, slots.astype(jnp.int32) - BIAS, EMPTY_SLOT)
    empty = jnp.where(filled, 0.0, EMPTY)[:most, :]
    for g in range(LANES // group):
        empty_ref[g] = pltpu.roll(empty, (LANES - g * group) % LANES, 1) if g else empty
    for k in range(0, LANES, 2):
        pair = [jnp.broadcast_to(slots[:most, k + j : k + j + 1], (most, LANES)) for j in range(2)]
        cs_ref[k * most : (k + 2) * most, :] = jnp.concatenate(pair, axis=0).astype(jnp.int16)


def own_sums(block, xcat_ref, crow_ref, cs_ref, sums_ref):
    chunks = crow_ref.shape[0]

    def step(m, carry):
        base = pl.multiple_of(m * block, block)
        cs = cs_ref[pl.ds(base, block), :]
        both = None
        for a in range(0, chunks, 2):
            parts = []
            for i in range(2):
                row = jnp.broadcast_to(crow_ref[a + i][None], (block // 16, 16, LANES)).reshape(block, LANES)
                parts.append(ones_where(cs - row < INSIDE))
            part = mm(jnp.concatenate(parts, axis=1), xcat_ref[a * LANES : (a + 2) * LANES, :])
            both = part if both is None else both + part
        sums_ref[pl.ds(base, block), :] = both[:, :LANES] + both[:, LANES:]
        return carry

    lax.fori_loop(0, cs_ref.shape[0] // block, step, 0)


def whole_kernel(
    nodes, most, group, rows_ref, mask_ref, keys_ref, gains_ref, got_ref,
    x_ref, m_ref, key_ref, gain_ref, tail_ref, tailin_ref, xcat_ref, crow_ref, c_ref, hits_ref, picks_ref,
    cs_ref, empty_ref, sums_ref, y_ref, sq_ref, sqin_ref,
    load_sems, tail_sems, swap_send, swap_recv, send_sem, recv_sem,
):
    me, rep = lax.axis_index("tm"), lax.axis_index("rep")
    barrier = pltpu.get_barrier_semaphore()
    loads = [
        pltpu.make_async_copy(source, target, load_sems.at[i])
        for i, (source, target) in enumerate(((mask_ref, m_ref), (keys_ref, key_ref), (rows_ref, x_ref), (gains_ref, gain_ref)))
    ]
    for load in loads:
        load.start()

    def greet(k, carry):
        pl.semaphore_signal(barrier, inc=1, device_id=(lax.rem(me + k, nodes), rep), device_id_type=MESH)
        return carry

    pl.semaphore_signal(barrier, inc=1, device_id=(me, 1 - rep), device_id_type=MESH)
    lax.fori_loop(1, nodes, greet, 0)
    loads[0].wait()
    find_tail(x_ref, m_ref[...], tail_ref, xcat_ref, crow_ref, c_ref, loads[2].wait)
    pl.semaphore_wait(barrier, nodes)
    onward = pltpu.make_async_remote_copy(
        src_ref=tail_ref,
        dst_ref=tailin_ref,
        send_sem=tail_sems.at[0],
        recv_sem=tail_sems.at[1],
        device_id=(lax.rem(me + 1, nodes), rep),
        device_id_type=MESH,
    )
    onward.start()
    loads[1].wait()
    find_slots(most, group, c_ref, key_ref, cs_ref, empty_ref, hits_ref, picks_ref)
    own_sums(group * most, xcat_ref, crow_ref, cs_ref, sums_ref)
    onward.wait()

    tail = tailin_ref[...]
    high = tail.astype(jnp.bfloat16)
    tailcat = jnp.concatenate([high, (tail - high.astype(jnp.float32)).astype(jnp.bfloat16)], axis=1)
    lanes = iota((most, LANES), 1)
    loads[3].wait()
    gain = gain_ref[...]
    size = group * most
    groups = nodes // group

    def place_of(j):
        return lax.rem(me // group + j, groups)

    def swap(j):
        return pltpu.make_async_remote_copy(
            src_ref=sq_ref.at[j],
            dst_ref=sqin_ref.at[j],
            send_sem=swap_send.at[j],
            recv_sem=swap_recv.at[j],
            device_id=(me, 1 - rep),
            device_id_type=MESH,
        )

    def add_tail(j):
        g = place_of(j)
        base = pl.multiple_of(g * size, size)
        cs = cs_ref[pl.ds(base, size), :]
        parts = [
            ones_where(cs - (iota((size, LANES), 1) + (a * LANES - WINDOW)).astype(jnp.int16) < INSIDE) for a in range(WINDOW // LANES)
        ]
        both = mm(jnp.concatenate(parts, axis=1), tailcat)
        y = sums_ref[pl.ds(base, size), :] + both[:, :LANES] + both[:, LANES:]
        y_ref[pl.ds(g * group, group)] = y.reshape(group, most, LANES)
        squares = jnp.sum(y * y, axis=1, keepdims=True)
        sq = jnp.zeros((most, LANES), jnp.float32)
        for i in range(group):
            sq = jnp.where(lanes == i, squares[i * most : (i + 1) * most, :], sq)
        sq_ref[j] = sq
        swap(j).start()

    def finish(j):
        g = place_of(j)
        swap(j).wait()
        inverse = 1.0 / jnp.sqrt((sq_ref[j] + sqin_ref[j]) / F + EPSILON)
        empty = empty_ref[g]
        for i in range(group):
            k = g * group + i
            y_ref[k] = y_ref[k] * gain * inverse[:, i : i + 1] + empty[:, i : i + 1]

        def send(i, carry):
            to = g * group + lax.rem(me + 1 + i, group)
            pltpu.make_async_remote_copy(
                src_ref=y_ref.at[to],
                dst_ref=got_ref.at[me],
                send_sem=send_sem,
                recv_sem=recv_sem,
                device_id=(to, rep),
                device_id_type=MESH,
            ).start()
            return carry

        lax.fori_loop(0, group - 1 if j == 0 else group, send, 0)

    add_tail(0)
    for j in range(1, groups):
        add_tail(j)
        finish(j - 1)
    finish(groups - 1)
    got_ref[me] = y_ref[me]
    others = pl.ds(0, nodes - 1)
    every = pltpu.make_async_remote_copy(
        src_ref=y_ref.at[others],
        dst_ref=got_ref.at[others],
        send_sem=send_sem,
        recv_sem=recv_sem,
        device_id=(me, 1 - rep),
        device_id_type=MESH,
    )
    every.wait_send()
    every.wait_recv()


def place_kernel(most, got_ref, out_ref, starts_v, starts_s, sem):
    nodes = got_ref.shape[0]
    size = nodes * most
    flags = as_bf16(got_ref[...].reshape(size, LANES) < LIMIT)
    slot = iota((nodes, size), 1)
    first = iota((nodes, size), 0) * most
    member = as_bf16((slot >= first) & (slot < first + most))
    counts = mm(member, flags)
    earlier = as_bf16(iota((nodes, nodes), 1) < iota((nodes, nodes), 0))
    starts = mm(earlier, counts.astype(jnp.bfloat16))
    diagonal = jnp.where(iota((nodes, LANES), 0) == iota((nodes, LANES), 1), starts, 0.0)
    starts_v[...] = jnp.sum(diagonal, axis=0, keepdims=True).astype(jnp.int32)
    copy = pltpu.make_async_copy(starts_v, starts_s, sem)
    copy.start()
    out_ref[...] = jnp.zeros_like(out_ref)
    copy.wait()

    for k in range(nodes):
        block = got_ref[k]
        out_ref[pl.ds(starts_s[0, k], most), :] = jnp.where(block < LIMIT, block, 0.0)


VMEM = pl.BlockSpec(memory_space=pltpu.VMEM)
HBM = pl.BlockSpec(memory_space=pltpu.HBM)


def call(kernel, name, outs, ins, scratch, megabytes, **settings):
    params = {"vmem_limit_bytes": megabytes << 20, **settings.pop("params", {})}
    return pl.pallas_call(
        kernel,
        out_shape=outs,
        in_specs=ins,
        out_specs=jax.tree.map(lambda _: VMEM, outs),
        scratch_shapes=scratch,
        compiler_params=pltpu.CompilerParams(**params),
        name=name,
        **settings,
    )


def local(rows, row_mask, key_bucket, gain):
    size_rows, half = rows.shape
    nodes = lax.axis_size("tm")
    most = 3 * size_rows // (4 * nodes)
    chunks = size_rows // LANES
    slots = nodes * most
    f32, bf16, i16, i32 = jnp.float32, jnp.bfloat16, jnp.int16, jnp.int32
    shape = jax.ShapeDtypeStruct
    dma = pltpu.SemaphoreType.DMA
    group = 32
    vmem = pltpu.VMEM
    in_hbm = functools.partial(pltpu.with_memory_space_constraint, memory_space=pltpu.HBM)
    got = call(
        functools.partial(whole_kernel, nodes, most, group),
        "whole",
        shape((nodes, most, half), f32),
        [HBM] * 4,
        [
            vmem((size_rows, half), f32),
            vmem((chunks, LANES), i32),
            vmem((chunks, LANES), i32),
            vmem((1, half), f32),
            vmem((WINDOW, half), f32),
            vmem((WINDOW, half), f32),
            vmem((size_rows, 2 * half), bf16),
            vmem((chunks, 16, LANES), i16),
            vmem((chunks, LANES), i32),
            vmem((nodes, size_rows), bf16),
            vmem((96, size_rows), bf16),
            vmem((slots, LANES), i16),
            vmem((nodes // group, most, LANES), f32),
            vmem((slots, half), f32),
            vmem((nodes, most, half), f32),
            vmem((nodes // group, most, LANES), f32),
            vmem((nodes // group, most, LANES), f32),
            dma((4,)),
            dma((2,)),
            dma((nodes // group,)),
            dma((nodes // group,)),
            dma,
            dma,
        ],
        40,
        params={"collective_id": 0, "has_side_effects": True},
    )(
        in_hbm(rows),
        in_hbm(row_mask.reshape(chunks, LANES)),
        in_hbm(key_bucket.reshape(chunks, LANES)),
        in_hbm(gain.reshape(1, half)),
    )
    return call(
        functools.partial(place_kernel, most),
        "place",
        shape((slots, half), f32),
        [VMEM],
        [pltpu.VMEM((1, LANES), i32), pltpu.SMEM((1, LANES), i32), dma],
        20,
    )(got)


def solution(mesh):
    in_specs = (P("tm", "rep"), P("tm"), P("tm"), P("rep"))
    out_specs = P("tm", "rep")
    return jax.shard_map(local, mesh=mesh, in_specs=in_specs, out_specs=out_specs, check_vma=False)
```

```python
import functools

import jax
import jax.numpy as jnp
from jax import lax
from jax.experimental import pallas as pl
from jax.experimental.pallas import tpu as pltpu
from jax.sharding import PartitionSpec as P

F = 256
WINDOW = 512
LANES = 128
EPSILON = 1e-06
MESH = pl.DeviceIdType.MESH

BIAS = 32768
INSIDE = WINDOW - BIAS
NOT_LIVE = 16384
EMPTY_SLOT = 16384
EMPTY = 1e9
LIMIT = 1e8


def iota(shape, dim):
    return lax.broadcasted_iota(jnp.int32, shape, dim)


def as_bf16(test):
    return jnp.where(test, jnp.float32(1.0), jnp.float32(0.0)).astype(jnp.bfloat16)


def ones_where(test):
    return jnp.where(test, jnp.bfloat16(1.0), jnp.bfloat16(0.0))


def mm(a, b):
    return jnp.dot(a, b, preferred_element_type=jnp.float32)


def split_rows(x_ref, xcat_ref, rows):
    x = x_ref[rows, :]
    high = x.astype(jnp.bfloat16)
    xcat_ref[rows, :LANES] = high
    xcat_ref[rows, LANES:] = (x - high.astype(jnp.float32)).astype(jnp.bfloat16)


def find_tail(first, x_ref, mask, tail_ref, xcat_ref, crow_ref, c_ref, wait_rows):
    size_rows = xcat_ref.shape[0]
    chunks = size_rows // LANES
    mask_bf = mask.astype(jnp.float32).astype(jnp.bfloat16)
    upper = as_bf16(iota((LANES, LANES), 0) <= iota((LANES, LANES), 1))
    within = mm(mask_bf, upper)
    totals = mm(mask_bf, jnp.ones((LANES, LANES), jnp.bfloat16))
    below = as_bf16(iota((chunks, chunks), 1) < iota((chunks, chunks), 0))
    before = mm(below, totals.astype(jnp.bfloat16))
    count = (before + totals)[chunks - 1 : chunks, :].astype(jnp.int32)
    c = jnp.where(mask == 1, (within + before - 1.0).astype(jnp.int32), NOT_LIVE)
    c_ref[...] = c
    rows16 = [jnp.broadcast_to(c[a : a + 1, :], (16, LANES)).astype(jnp.int16) for a in range(chunks)]
    for a in range(chunks):
        crow_ref[a] = rows16[a]
    wait_rows()
    split_rows(x_ref, xcat_ref, slice(first * LANES, size_rows))
    wanted = jnp.broadcast_to(count - WINDOW, (WINDOW, LANES)) + iota((WINDOW, LANES), 0)
    wanted = wanted.astype(jnp.int16)
    parts = []
    for a in range(first, chunks):
        parts.append(ones_where(wanted == jnp.broadcast_to(rows16[a][None], (WINDOW // 16, 16, LANES)).reshape(WINDOW, LANES)))
    both = mm(jnp.concatenate(parts, axis=1), xcat_ref[first * LANES :, :])
    tail_ref[...] = both[:, :LANES] + both[:, LANES:]


def find_slots(most, group, c_ref, key_ref, cs_ref, empty_ref, hits_ref, picks_ref):
    chunks = c_ref.shape[0]
    c = c_ref[...]
    key = jnp.where(c < NOT_LIVE, key_ref[...], -1)
    buckets = iota((LANES, LANES), 0)
    for a in range(chunks):
        hits_ref[:, a * LANES : (a + 1) * LANES] = as_bf16(jnp.broadcast_to(key[a : a + 1, :], (LANES, LANES)) == buckets)
    upper = as_bf16(iota((256, 256), 0) <= iota((256, 256), 1))
    carry = jnp.zeros((LANES, 1), jnp.float32)
    ranks = iota((32, LANES), 0)
    for b in range(chunks // 2):
        hits = hits_ref[:, b * 256 : (b + 1) * 256]
        running = mm(hits, upper)
        rank = jnp.sum(hits.astype(jnp.float32) * (running + carry), axis=0, keepdims=True) - 1.0
        carry = carry + running[:, 255:256]
        for h in range(2):
            a = 2 * b + h
            same = jnp.broadcast_to(rank[:, h * LANES : (h + 1) * LANES], (32, LANES)).astype(jnp.int32) == ranks
            high = jnp.broadcast_to((c[a : a + 1, :] >> 6).astype(jnp.float32), (32, LANES))
            low = jnp.broadcast_to((c[a : a + 1, :] & 63).astype(jnp.float32), (32, LANES))
            place = slice(a * LANES, (a + 1) * LANES)
            picks_ref[0:32, place] = jnp.where(same, high, 0.0).astype(jnp.bfloat16)
            picks_ref[32:64, place] = jnp.where(same, low, 0.0).astype(jnp.bfloat16)
            picks_ref[64:96, place] = jnp.where(same, 1.0, 0.0).astype(jnp.bfloat16)
    found = lax.dot_general(picks_ref[...], hits_ref[...], (((1,), (1,)), ((), ())), preferred_element_type=jnp.float32)
    filled = found[64:96, :] > 0.5
    slots = found[0:32, :] * 64.0 + found[32:64, :]
    slots = jnp.where(filled, slots.astype(jnp.int32) - BIAS, EMPTY_SLOT)
    empty = jnp.where(filled, 0.0, EMPTY)[:most, :]
    for g in range(LANES // group):
        empty_ref[g] = pltpu.roll(empty, (LANES - g * group) % LANES, 1) if g else empty
    for k in range(0, LANES, 2):
        pair = [jnp.broadcast_to(slots[:most, k + j : k + j + 1], (most, LANES)) for j in range(2)]
        cs_ref[k * most : (k + 2) * most, :] = jnp.concatenate(pair, axis=0).astype(jnp.int16)


def own_sums(block, first_j, last_j, place_of, xcat_ref, crow_ref, cs_ref, sums_ref):
    chunks = crow_ref.shape[0]

    def step(j, carry):
        base = pl.multiple_of(place_of(j) * block, block)
        cs = cs_ref[pl.ds(base, block), :]
        both = None
        for a in range(0, chunks, 2):
            parts = []
            for i in range(2):
                row = jnp.broadcast_to(crow_ref[a + i][None], (block // 16, 16, LANES)).reshape(block, LANES)
                parts.append(ones_where(cs - row < INSIDE))
            part = mm(jnp.concatenate(parts, axis=1), xcat_ref[a * LANES : (a + 2) * LANES, :])
            both = part if both is None else both + part
        sums_ref[pl.ds(base, block), :] = both[:, :LANES] + both[:, LANES:]
        return carry

    lax.fori_loop(first_j, last_j, step, 0)


def whole_kernel(
    nodes, most, group, rows_ref, mask_ref, keys_ref, gains_ref, got_ref,
    x_ref, m_ref, key_ref, gain_ref, tail_ref, tailin_ref, xcat_ref, crow_ref, c_ref, hits_ref, picks_ref,
    cs_ref, empty_ref, sums_ref, y_ref, sq_ref, sqin_ref,
    load_sems, tail_sems, swap_send, swap_recv, send_sem, recv_sem,
):
    me, rep = lax.axis_index("tm"), lax.axis_index("rep")
    barrier = pltpu.get_barrier_semaphore()
    size_rows = x_ref.shape[0]
    first = (size_rows // 2 - WINDOW) // LANES
    early, late = slice(0, first * LANES), slice(first * LANES, size_rows)
    pairs = (
        (mask_ref, m_ref),
        (rows_ref.at[late, :], x_ref.at[late, :]),
        (keys_ref, key_ref),
        (rows_ref.at[early, :], x_ref.at[early, :]),
        (gains_ref, gain_ref),
    )
    loads = [pltpu.make_async_copy(source, target, load_sems.at[i]) for i, (source, target) in enumerate(pairs)]
    for load in loads:
        load.start()

    def greet(k, carry):
        pl.semaphore_signal(barrier, inc=1, device_id=(lax.rem(me + k, nodes), rep), device_id_type=MESH)
        return carry

    pl.semaphore_signal(barrier, inc=1, device_id=(me, 1 - rep), device_id_type=MESH)
    lax.fori_loop(1, nodes, greet, 0)
    loads[0].wait()
    find_tail(first, x_ref, m_ref[...], tail_ref, xcat_ref, crow_ref, c_ref, loads[1].wait)
    pl.semaphore_wait(barrier, nodes)
    onward = pltpu.make_async_remote_copy(
        src_ref=tail_ref,
        dst_ref=tailin_ref,
        send_sem=tail_sems.at[0],
        recv_sem=tail_sems.at[1],
        device_id=(lax.rem(me + 1, nodes), rep),
        device_id_type=MESH,
    )
    onward.start()
    loads[2].wait()
    find_slots(most, group, c_ref, key_ref, cs_ref, empty_ref, hits_ref, picks_ref)
    loads[3].wait()
    split_rows(x_ref, xcat_ref, early)
    size = group * most
    groups = nodes // group

    def place_of(j):
        return lax.rem(me // group + j, groups)

    def own(first_j, last_j):
        own_sums(size, first_j, last_j, place_of, xcat_ref, crow_ref, cs_ref, sums_ref)

    own(0, groups - 1)
    onward.wait()

    tail = tailin_ref[...]
    high = tail.astype(jnp.bfloat16)
    tailcat = jnp.concatenate([high, (tail - high.astype(jnp.float32)).astype(jnp.bfloat16)], axis=1)
    lanes = iota((most, LANES), 1)
    loads[4].wait()
    gain = gain_ref[...]

    def swap(j):
        return pltpu.make_async_remote_copy(
            src_ref=sq_ref.at[j],
            dst_ref=sqin_ref.at[j],
            send_sem=swap_send.at[j],
            recv_sem=swap_recv.at[j],
            device_id=(me, 1 - rep),
            device_id_type=MESH,
        )

    def add_tail(j):
        g = place_of(j)
        base = pl.multiple_of(g * size, size)
        cs = cs_ref[pl.ds(base, size), :]
        parts = [
            ones_where(cs - (iota((size, LANES), 1) + (a * LANES - WINDOW)).astype(jnp.int16) < INSIDE) for a in range(WINDOW // LANES)
        ]
        both = mm(jnp.concatenate(parts, axis=1), tailcat)
        y = sums_ref[pl.ds(base, size), :] + both[:, :LANES] + both[:, LANES:]
        y_ref[pl.ds(g * group, group)] = y.reshape(group, most, LANES)
        squares = jnp.sum(y * y, axis=1, keepdims=True)
        sq = jnp.zeros((most, LANES), jnp.float32)
        for i in range(group):
            sq = jnp.where(lanes == i, squares[i * most : (i + 1) * most, :], sq)
        sq_ref[j] = sq
        swap(j).start()

    def finish(j):
        g = place_of(j)
        swap(j).wait()
        inverse = 1.0 / jnp.sqrt((sq_ref[j] + sqin_ref[j]) / F + EPSILON)
        empty = empty_ref[g]
        for i in range(group):
            k = g * group + i
            y_ref[k] = y_ref[k] * gain * inverse[:, i : i + 1] + empty[:, i : i + 1]

        def send(i, carry):
            to = g * group + lax.rem(me + 1 + i, group)
            pltpu.make_async_remote_copy(
                src_ref=y_ref.at[to],
                dst_ref=got_ref.at[me],
                send_sem=send_sem,
                recv_sem=recv_sem,
                device_id=(to, rep),
                device_id_type=MESH,
            ).start()
            return carry

        lax.fori_loop(0, group - 1 if j == 0 else group, send, 0)

    add_tail(0)
    for j in range(1, groups - 1):
        add_tail(j)
        finish(j - 1)
    own(groups - 1, groups)
    finish(groups - 2)
    add_tail(groups - 1)
    finish(groups - 1)
    got_ref[me] = y_ref[me]
    others = pl.ds(0, nodes - 1)
    every = pltpu.make_async_remote_copy(
        src_ref=y_ref.at[others],
        dst_ref=got_ref.at[others],
        send_sem=send_sem,
        recv_sem=recv_sem,
        device_id=(me, 1 - rep),
        device_id_type=MESH,
    )
    every.wait_send()
    every.wait_recv()


def place_kernel(most, got_ref, out_ref, starts_v, starts_s, sem):
    nodes = got_ref.shape[0]
    size = nodes * most
    flags = as_bf16(got_ref[...].reshape(size, LANES) < LIMIT)
    slot = iota((nodes, size), 1)
    first = iota((nodes, size), 0) * most
    member = as_bf16((slot >= first) & (slot < first + most))
    counts = mm(member, flags)
    earlier = as_bf16(iota((nodes, nodes), 1) < iota((nodes, nodes), 0))
    starts = mm(earlier, counts.astype(jnp.bfloat16))
    diagonal = jnp.where(iota((nodes, LANES), 0) == iota((nodes, LANES), 1), starts, 0.0)
    starts_v[...] = jnp.sum(diagonal, axis=0, keepdims=True).astype(jnp.int32)
    copy = pltpu.make_async_copy(starts_v, starts_s, sem)
    copy.start()
    out_ref[...] = jnp.zeros_like(out_ref)
    copy.wait()

    for k in range(nodes):
        block = got_ref[k]
        out_ref[pl.ds(starts_s[0, k], most), :] = jnp.where(block < LIMIT, block, 0.0)


VMEM = pl.BlockSpec(memory_space=pltpu.VMEM)
HBM = pl.BlockSpec(memory_space=pltpu.HBM)


def call(kernel, name, outs, ins, scratch, megabytes, **settings):
    params = {"vmem_limit_bytes": megabytes << 20, **settings.pop("params", {})}
    return pl.pallas_call(
        kernel,
        out_shape=outs,
        in_specs=ins,
        out_specs=jax.tree.map(lambda _: VMEM, outs),
        scratch_shapes=scratch,
        compiler_params=pltpu.CompilerParams(**params),
        name=name,
        **settings,
    )


def local(rows, row_mask, key_bucket, gain):
    size_rows, half = rows.shape
    nodes = lax.axis_size("tm")
    most = 3 * size_rows // (4 * nodes)
    chunks = size_rows // LANES
    slots = nodes * most
    f32, bf16, i16, i32 = jnp.float32, jnp.bfloat16, jnp.int16, jnp.int32
    shape = jax.ShapeDtypeStruct
    dma = pltpu.SemaphoreType.DMA
    group = 32
    vmem = pltpu.VMEM
    in_hbm = functools.partial(pltpu.with_memory_space_constraint, memory_space=pltpu.HBM)
    got = call(
        functools.partial(whole_kernel, nodes, most, group),
        "whole",
        shape((nodes, most, half), f32),
        [HBM] * 4,
        [
            vmem((size_rows, half), f32),
            vmem((chunks, LANES), i32),
            vmem((chunks, LANES), i32),
            vmem((1, half), f32),
            vmem((WINDOW, half), f32),
            vmem((WINDOW, half), f32),
            vmem((size_rows, 2 * half), bf16),
            vmem((chunks, 16, LANES), i16),
            vmem((chunks, LANES), i32),
            vmem((nodes, size_rows), bf16),
            vmem((96, size_rows), bf16),
            vmem((slots, LANES), i16),
            vmem((nodes // group, most, LANES), f32),
            vmem((slots, half), f32),
            vmem((nodes, most, half), f32),
            vmem((nodes // group, most, LANES), f32),
            vmem((nodes // group, most, LANES), f32),
            dma((5,)),
            dma((2,)),
            dma((nodes // group,)),
            dma((nodes // group,)),
            dma,
            dma,
        ],
        40,
        params={"collective_id": 0, "has_side_effects": True},
    )(
        in_hbm(rows),
        in_hbm(row_mask.reshape(chunks, LANES)),
        in_hbm(key_bucket.reshape(chunks, LANES)),
        in_hbm(gain.reshape(1, half)),
    )
    return call(
        functools.partial(place_kernel, most),
        "place",
        shape((slots, half), f32),
        [VMEM],
        [pltpu.VMEM((1, LANES), i32), pltpu.SMEM((1, LANES), i32), dma],
        20,
    )(got)


def solution(mesh):
    in_specs = (P("tm", "rep"), P("tm"), P("tm"), P("rep"))
    out_specs = P("tm", "rep")
    return jax.shard_map(local, mesh=mesh, in_specs=in_specs, out_specs=out_specs, check_vma=False)
```

```python
import functools

import jax
import jax.numpy as jnp
from jax import lax
from jax.experimental import pallas as pl
from jax.experimental.pallas import tpu as pltpu
from jax.sharding import PartitionSpec as P

F = 256
WINDOW = 512
LANES = 128
EPSILON = 1e-06
TAIL_PARTS = 2
MESH = pl.DeviceIdType.MESH

BIAS = 32768
INSIDE = WINDOW - BIAS
NOT_LIVE = 16384
EMPTY_SLOT = 16384
EMPTY = 1e9
LIMIT = 1e8


def iota(shape, dim):
    return lax.broadcasted_iota(jnp.int32, shape, dim)


def as_bf16(test):
    return jnp.where(test, jnp.float32(1.0), jnp.float32(0.0)).astype(jnp.bfloat16)


def ones_where(test):
    return jnp.where(test, jnp.bfloat16(1.0), jnp.bfloat16(0.0))


def mm(a, b):
    return jnp.dot(a, b, preferred_element_type=jnp.float32)


def split_rows(x_ref, xcat_ref, rows):
    x = x_ref[rows, :]
    high = x.astype(jnp.bfloat16)
    xcat_ref[rows, :LANES] = high
    xcat_ref[rows, LANES:] = (x - high.astype(jnp.float32)).astype(jnp.bfloat16)


def find_tail(first, x_ref, mask, tail_ref, xcat_ref, crow_ref, c_ref, wait_rows):
    size_rows = xcat_ref.shape[0]
    chunks = size_rows // LANES
    mask_bf = mask.astype(jnp.float32).astype(jnp.bfloat16)
    upper = as_bf16(iota((LANES, LANES), 0) <= iota((LANES, LANES), 1))
    within = mm(mask_bf, upper)
    totals = mm(mask_bf, jnp.ones((LANES, LANES), jnp.bfloat16))
    below = as_bf16(iota((chunks, chunks), 1) < iota((chunks, chunks), 0))
    before = mm(below, totals.astype(jnp.bfloat16))
    count = (before + totals)[chunks - 1 : chunks, :].astype(jnp.int32)
    c = jnp.where(mask == 1, (within + before - 1.0).astype(jnp.int32), NOT_LIVE)
    c_ref[...] = c
    rows16 = [jnp.broadcast_to(c[a : a + 1, :], (16, LANES)).astype(jnp.int16) for a in range(chunks)]
    for a in range(chunks):
        crow_ref[a] = rows16[a]
    wait_rows()
    split_rows(x_ref, xcat_ref, slice(first * LANES, size_rows))
    size = WINDOW // TAIL_PARTS

    def part(h):
        wanted = jnp.broadcast_to(count - WINDOW + h * size, (size, LANES)) + iota((size, LANES), 0)
        wanted = wanted.astype(jnp.int16)
        parts = []
        for a in range(first, chunks):
            parts.append(ones_where(wanted == jnp.broadcast_to(rows16[a][None], (size // 16, 16, LANES)).reshape(size, LANES)))
        both = mm(jnp.concatenate(parts, axis=1), xcat_ref[first * LANES :, :])
        tail_ref[h] = both[:, :LANES] + both[:, LANES:]

    return part


def find_slots(most, group, c_ref, key_ref, cs_ref, empty_ref, hits_ref, picks_ref):
    chunks = c_ref.shape[0]
    c = c_ref[...]
    key = jnp.where(c < NOT_LIVE, key_ref[...], -1)
    buckets = iota((LANES, LANES), 0)
    for a in range(chunks):
        hits_ref[:, a * LANES : (a + 1) * LANES] = as_bf16(jnp.broadcast_to(key[a : a + 1, :], (LANES, LANES)) == buckets)
    upper = as_bf16(iota((256, 256), 0) <= iota((256, 256), 1))
    carry = jnp.zeros((LANES, 1), jnp.float32)
    ranks = iota((32, LANES), 0)
    for b in range(chunks // 2):
        hits = hits_ref[:, b * 256 : (b + 1) * 256]
        running = mm(hits, upper)
        rank = jnp.sum(hits.astype(jnp.float32) * (running + carry), axis=0, keepdims=True) - 1.0
        carry = carry + running[:, 255:256]
        for h in range(2):
            a = 2 * b + h
            same = jnp.broadcast_to(rank[:, h * LANES : (h + 1) * LANES], (32, LANES)).astype(jnp.int32) == ranks
            high = jnp.broadcast_to((c[a : a + 1, :] >> 6).astype(jnp.float32), (32, LANES))
            low = jnp.broadcast_to((c[a : a + 1, :] & 63).astype(jnp.float32), (32, LANES))
            place = slice(a * LANES, (a + 1) * LANES)
            picks_ref[0:32, place] = jnp.where(same, high, 0.0).astype(jnp.bfloat16)
            picks_ref[32:64, place] = jnp.where(same, low, 0.0).astype(jnp.bfloat16)
            picks_ref[64:96, place] = jnp.where(same, 1.0, 0.0).astype(jnp.bfloat16)
    found = lax.dot_general(picks_ref[...], hits_ref[...], (((1,), (1,)), ((), ())), preferred_element_type=jnp.float32)
    filled = found[64:96, :] > 0.5
    slots = found[0:32, :] * 64.0 + found[32:64, :]
    slots = jnp.where(filled, slots.astype(jnp.int32) - BIAS, EMPTY_SLOT)
    empty = jnp.where(filled, 0.0, EMPTY)[:most, :]
    for g in range(LANES // group):
        empty_ref[g] = pltpu.roll(empty, (LANES - g * group) % LANES, 1) if g else empty
    for k in range(0, LANES, 2):
        pair = [jnp.broadcast_to(slots[:most, k + j : k + j + 1], (most, LANES)) for j in range(2)]
        cs_ref[k * most : (k + 2) * most, :] = jnp.concatenate(pair, axis=0).astype(jnp.int16)


def own_sums(block, first_j, last_j, place_of, xcat_ref, crow_ref, cs_ref, sums_ref):
    chunks = crow_ref.shape[0]

    def step(j, carry):
        base = pl.multiple_of(place_of(j) * block, block)
        cs = cs_ref[pl.ds(base, block), :]
        both = None
        for a in range(0, chunks, 2):
            parts = []
            for i in range(2):
                row = jnp.broadcast_to(crow_ref[a + i][None], (block // 16, 16, LANES)).reshape(block, LANES)
                parts.append(ones_where(cs - row < INSIDE))
            part = mm(jnp.concatenate(parts, axis=1), xcat_ref[a * LANES : (a + 2) * LANES, :])
            both = part if both is None else both + part
        sums_ref[pl.ds(base, block), :] = both[:, :LANES] + both[:, LANES:]
        return carry

    lax.fori_loop(first_j, last_j, step, 0)


def whole_kernel(
    nodes, most, group, rows_ref, mask_ref, keys_ref, gains_ref, got_ref,
    x_ref, m_ref, key_ref, gain_ref, tail_ref, tailin_ref, xcat_ref, crow_ref, c_ref, hits_ref, picks_ref,
    cs_ref, empty_ref, sums_ref, y_ref, sq_ref, sqin_ref,
    load_sems, tail_send, tail_recv, swap_send, swap_recv, send_sem, recv_sem,
):
    me, rep = lax.axis_index("tm"), lax.axis_index("rep")
    barrier = pltpu.get_barrier_semaphore()
    size_rows = x_ref.shape[0]
    first = (size_rows // 2 - WINDOW) // LANES
    early, late = slice(0, first * LANES), slice(first * LANES, size_rows)
    pairs = (
        (mask_ref, m_ref),
        (rows_ref.at[late, :], x_ref.at[late, :]),
        (keys_ref, key_ref),
        (rows_ref.at[early, :], x_ref.at[early, :]),
        (gains_ref, gain_ref),
    )
    loads = [pltpu.make_async_copy(source, target, load_sems.at[i]) for i, (source, target) in enumerate(pairs)]
    for i in (0, 1, 2, 4):
        loads[i].start()

    def greet(k, carry):
        pl.semaphore_signal(barrier, inc=1, device_id=(lax.rem(me + k, nodes), rep), device_id_type=MESH)
        return carry

    pl.semaphore_signal(barrier, inc=1, device_id=(me, 1 - rep), device_id_type=MESH)
    lax.fori_loop(1, nodes, greet, 0)
    loads[0].wait()
    tail_part = find_tail(first, x_ref, m_ref[...], tail_ref, xcat_ref, crow_ref, c_ref, loads[1].wait)

    def onward(h):
        return pltpu.make_async_remote_copy(
            src_ref=tail_ref.at[h],
            dst_ref=tailin_ref.at[h],
            send_sem=tail_send.at[h],
            recv_sem=tail_recv.at[h],
            device_id=(lax.rem(me + 1, nodes), rep),
            device_id_type=MESH,
        )

    for h in range(TAIL_PARTS):
        tail_part(h)
        if h == 0:
            pl.semaphore_wait(barrier, nodes)
        if h == TAIL_PARTS - 1:
            loads[3].start()
            loads[2].wait()
        onward(h).start()
    find_slots(most, group, c_ref, key_ref, cs_ref, empty_ref, hits_ref, picks_ref)
    loads[3].wait()
    split_rows(x_ref, xcat_ref, early)
    size = group * most
    groups = nodes // group

    def place_of(j):
        return lax.rem(me // group + j, groups)

    def own(first_j, last_j):
        own_sums(size, first_j, last_j, place_of, xcat_ref, crow_ref, cs_ref, sums_ref)

    own(0, groups - 1)
    for h in range(TAIL_PARTS):
        onward(h).wait()

    tail = tailin_ref[...].reshape(WINDOW, LANES)
    high = tail.astype(jnp.bfloat16)
    tailcat = jnp.concatenate([high, (tail - high.astype(jnp.float32)).astype(jnp.bfloat16)], axis=1)
    lanes = iota((most, LANES), 1)
    loads[4].wait()
    gain = gain_ref[...]

    def swap(j):
        return pltpu.make_async_remote_copy(
            src_ref=sq_ref.at[j],
            dst_ref=sqin_ref.at[j],
            send_sem=swap_send.at[j],
            recv_sem=swap_recv.at[j],
            device_id=(me, 1 - rep),
            device_id_type=MESH,
        )

    def add_tail(j):
        g = place_of(j)
        base = pl.multiple_of(g * size, size)
        cs = cs_ref[pl.ds(base, size), :]
        parts = [
            ones_where(cs - (iota((size, LANES), 1) + (a * LANES - WINDOW)).astype(jnp.int16) < INSIDE) for a in range(WINDOW // LANES)
        ]
        both = mm(jnp.concatenate(parts, axis=1), tailcat)
        y = sums_ref[pl.ds(base, size), :] + both[:, :LANES] + both[:, LANES:]
        y_ref[pl.ds(g * group, group)] = y.reshape(group, most, LANES)
        squares = jnp.sum(y * y, axis=1, keepdims=True)
        sq = jnp.zeros((most, LANES), jnp.float32)
        for i in range(group):
            sq = jnp.where(lanes == i, squares[i * most : (i + 1) * most, :], sq)
        sq_ref[j] = sq
        swap(j).start()

    def finish(j):
        g = place_of(j)
        swap(j).wait()
        inverse = 1.0 / jnp.sqrt((sq_ref[j] + sqin_ref[j]) / F + EPSILON)
        empty = empty_ref[g]
        for i in range(group):
            k = g * group + i
            y_ref[k] = y_ref[k] * gain * inverse[:, i : i + 1] + empty[:, i : i + 1]

        def send(i, carry):
            to = g * group + lax.rem(me + 1 + i, group)
            pltpu.make_async_remote_copy(
                src_ref=y_ref.at[to],
                dst_ref=got_ref.at[me],
                send_sem=send_sem,
                recv_sem=recv_sem,
                device_id=(to, rep),
                device_id_type=MESH,
            ).start()
            return carry

        lax.fori_loop(0, group - 1 if j == 0 else group, send, 0)

    add_tail(0)
    for j in range(1, groups - 1):
        add_tail(j)
        finish(j - 1)
    own(groups - 1, groups)
    finish(groups - 2)
    add_tail(groups - 1)
    finish(groups - 1)
    got_ref[me] = y_ref[me]
    others = pl.ds(0, nodes - 1)
    every = pltpu.make_async_remote_copy(
        src_ref=y_ref.at[others],
        dst_ref=got_ref.at[others],
        send_sem=send_sem,
        recv_sem=recv_sem,
        device_id=(me, 1 - rep),
        device_id_type=MESH,
    )
    every.wait_send()
    every.wait_recv()


def place_kernel(most, got_ref, out_ref, starts_v, starts_s, sem):
    nodes = got_ref.shape[0]
    counts = jnp.sum(jnp.where(got_ref[...] < LIMIT, 1.0, 0.0), axis=1)
    earlier = as_bf16(iota((nodes, nodes), 1) < iota((nodes, nodes), 0))
    starts = mm(earlier, counts.astype(jnp.bfloat16))
    diagonal = jnp.where(iota((nodes, LANES), 0) == iota((nodes, LANES), 1), starts, 0.0)
    starts_v[...] = jnp.sum(diagonal, axis=0, keepdims=True).astype(jnp.int32)
    copy = pltpu.make_async_copy(starts_v, starts_s, sem)
    copy.start()
    out_ref[...] = jnp.zeros_like(out_ref)
    copy.wait()

    for k in range(nodes):
        block = got_ref[k]
        out_ref[pl.ds(starts_s[0, k], most), :] = jnp.where(block < LIMIT, block, 0.0)


VMEM = pl.BlockSpec(memory_space=pltpu.VMEM)
HBM = pl.BlockSpec(memory_space=pltpu.HBM)


def call(kernel, name, outs, ins, scratch, megabytes, **settings):
    params = {"vmem_limit_bytes": megabytes << 20, **settings.pop("params", {})}
    return pl.pallas_call(
        kernel,
        out_shape=outs,
        in_specs=ins,
        out_specs=jax.tree.map(lambda _: VMEM, outs),
        scratch_shapes=scratch,
        compiler_params=pltpu.CompilerParams(**params),
        name=name,
        **settings,
    )


def local(rows, row_mask, key_bucket, gain):
    size_rows, half = rows.shape
    nodes = lax.axis_size("tm")
    most = 3 * size_rows // (4 * nodes)
    chunks = size_rows // LANES
    slots = nodes * most
    f32, bf16, i16, i32 = jnp.float32, jnp.bfloat16, jnp.int16, jnp.int32
    shape = jax.ShapeDtypeStruct
    dma = pltpu.SemaphoreType.DMA
    group = 32
    vmem = pltpu.VMEM
    in_hbm = functools.partial(pltpu.with_memory_space_constraint, memory_space=pltpu.HBM)
    got = call(
        functools.partial(whole_kernel, nodes, most, group),
        "whole",
        shape((nodes, most, half), f32),
        [HBM] * 4,
        [
            vmem((size_rows, half), f32),
            vmem((chunks, LANES), i32),
            vmem((chunks, LANES), i32),
            vmem((1, half), f32),
            vmem((TAIL_PARTS, WINDOW // TAIL_PARTS, half), f32),
            vmem((TAIL_PARTS, WINDOW // TAIL_PARTS, half), f32),
            vmem((size_rows, 2 * half), bf16),
            vmem((chunks, 16, LANES), i16),
            vmem((chunks, LANES), i32),
            vmem((nodes, size_rows), bf16),
            vmem((96, size_rows), bf16),
            vmem((slots, LANES), i16),
            vmem((nodes // group, most, LANES), f32),
            vmem((slots, half), f32),
            vmem((nodes, most, half), f32),
            vmem((nodes // group, most, LANES), f32),
            vmem((nodes // group, most, LANES), f32),
            dma((5,)),
            dma((TAIL_PARTS,)),
            dma((TAIL_PARTS,)),
            dma((nodes // group,)),
            dma((nodes // group,)),
            dma,
            dma,
        ],
        40,
        params={"collective_id": 0, "has_side_effects": True},
    )(
        in_hbm(rows),
        in_hbm(row_mask.reshape(chunks, LANES)),
        in_hbm(key_bucket.reshape(chunks, LANES)),
        in_hbm(gain.reshape(1, half)),
    )
    return call(
        functools.partial(place_kernel, most),
        "place",
        shape((slots, half), f32),
        [VMEM],
        [pltpu.VMEM((1, LANES), i32), pltpu.SMEM((1, LANES), i32), dma],
        20,
    )(got)


def solution(mesh):
    in_specs = (P("tm", "rep"), P("tm"), P("tm"), P("rep"))
    out_specs = P("tm", "rep")
    return jax.shard_map(local, mesh=mesh, in_specs=in_specs, out_specs=out_specs, check_vma=False)
```

```python
import functools

import jax
import jax.numpy as jnp
from jax import lax
from jax.experimental import pallas as pl
from jax.experimental.pallas import tpu as pltpu
from jax.sharding import PartitionSpec as P

F = 256
WINDOW = 512
LANES = 128
EPSILON = 1e-06
TAIL_PARTS = 1
MESH = pl.DeviceIdType.MESH

BIAS = 32768
INSIDE = WINDOW - BIAS
NOT_LIVE = 16384
EMPTY_SLOT = 16384
EMPTY = 1e9
LIMIT = 1e8


def iota(shape, dim):
    return lax.broadcasted_iota(jnp.int32, shape, dim)


def as_bf16(test):
    return jnp.where(test, jnp.float32(1.0), jnp.float32(0.0)).astype(jnp.bfloat16)


def ones_where(test):
    return jnp.where(test, jnp.bfloat16(1.0), jnp.bfloat16(0.0))


def mm(a, b):
    return jnp.dot(a, b, preferred_element_type=jnp.float32)


def split_rows(x_ref, xcat_ref, rows):
    x = x_ref[rows, :]
    high = x.astype(jnp.bfloat16)
    xcat_ref[rows, :LANES] = high
    xcat_ref[rows, LANES:] = (x - high.astype(jnp.float32)).astype(jnp.bfloat16)


def find_tail(first, x_ref, mask, tail_ref, xcat_ref, crow_ref, c_ref, wait_rows):
    size_rows = xcat_ref.shape[0]
    chunks = size_rows // LANES
    mask_bf = mask.astype(jnp.float32).astype(jnp.bfloat16)
    upper = as_bf16(iota((LANES, LANES), 0) <= iota((LANES, LANES), 1))
    within = mm(mask_bf, upper)
    totals = mm(mask_bf, jnp.ones((LANES, LANES), jnp.bfloat16))
    below = as_bf16(iota((chunks, chunks), 1) < iota((chunks, chunks), 0))
    before = mm(below, totals.astype(jnp.bfloat16))
    count = (before + totals)[chunks - 1 : chunks, :].astype(jnp.int32)
    c = jnp.where(mask == 1, (within + before - 1.0).astype(jnp.int32), NOT_LIVE)
    c_ref[...] = c
    rows16 = [jnp.broadcast_to(c[a : a + 1, :], (16, LANES)).astype(jnp.int16) for a in range(chunks)]
    for a in range(chunks):
        crow_ref[a] = rows16[a]
    wait_rows()
    split_rows(x_ref, xcat_ref, slice(first * LANES, size_rows))
    size = WINDOW // TAIL_PARTS

    def part(h):
        wanted = jnp.broadcast_to(count - WINDOW + h * size, (size, LANES)) + iota((size, LANES), 0)
        wanted = wanted.astype(jnp.int16)
        parts = []
        for a in range(first, chunks):
            parts.append(ones_where(wanted == jnp.broadcast_to(rows16[a][None], (size // 16, 16, LANES)).reshape(size, LANES)))
        both = mm(jnp.concatenate(parts, axis=1), xcat_ref[first * LANES :, :])
        tail_ref[h] = both[:, :LANES] + both[:, LANES:]

    return part


def find_slots(most, group, c_ref, key_ref, cs_ref, empty_ref, hits_ref, picks_ref):
    chunks = c_ref.shape[0]
    c = c_ref[...]
    key = jnp.where(c < NOT_LIVE, key_ref[...], -1)
    buckets = iota((LANES, LANES), 0)
    for a in range(chunks):
        hits_ref[:, a * LANES : (a + 1) * LANES] = as_bf16(jnp.broadcast_to(key[a : a + 1, :], (LANES, LANES)) == buckets)
    upper = as_bf16(iota((256, 256), 0) <= iota((256, 256), 1))
    carry = jnp.zeros((LANES, 1), jnp.float32)
    ranks = iota((32, LANES), 0)
    for b in range(chunks // 2):
        hits = hits_ref[:, b * 256 : (b + 1) * 256]
        running = mm(hits, upper)
        rank = jnp.sum(hits.astype(jnp.float32) * (running + carry), axis=0, keepdims=True) - 1.0
        carry = carry + running[:, 255:256]
        for h in range(2):
            a = 2 * b + h
            same = jnp.broadcast_to(rank[:, h * LANES : (h + 1) * LANES], (32, LANES)).astype(jnp.int32) == ranks
            high = jnp.broadcast_to((c[a : a + 1, :] >> 6).astype(jnp.float32), (32, LANES))
            low = jnp.broadcast_to((c[a : a + 1, :] & 63).astype(jnp.float32), (32, LANES))
            place = slice(a * LANES, (a + 1) * LANES)
            picks_ref[0:32, place] = jnp.where(same, high, 0.0).astype(jnp.bfloat16)
            picks_ref[32:64, place] = jnp.where(same, low, 0.0).astype(jnp.bfloat16)
            picks_ref[64:96, place] = jnp.where(same, 1.0, 0.0).astype(jnp.bfloat16)
    found = lax.dot_general(picks_ref[...], hits_ref[...], (((1,), (1,)), ((), ())), preferred_element_type=jnp.float32)
    filled = found[64:96, :] > 0.5
    slots = found[0:32, :] * 64.0 + found[32:64, :]
    slots = jnp.where(filled, slots.astype(jnp.int32) - BIAS, EMPTY_SLOT)
    empty = jnp.where(filled, 0.0, EMPTY)[:most, :]
    for g in range(LANES // group):
        empty_ref[g] = pltpu.roll(empty, (LANES - g * group) % LANES, 1) if g else empty
    for k in range(0, LANES, 2):
        pair = [jnp.broadcast_to(slots[:most, k + j : k + j + 1], (most, LANES)) for j in range(2)]
        cs_ref[k * most : (k + 2) * most, :] = jnp.concatenate(pair, axis=0).astype(jnp.int16)


def own_sums(block, first_j, last_j, place_of, xcat_ref, crow_ref, cs_ref, sums_ref):
    chunks = crow_ref.shape[0]

    def step(j, carry):
        base = pl.multiple_of(place_of(j) * block, block)
        cs = cs_ref[pl.ds(base, block), :]
        both = None
        for a in range(0, chunks, 2):
            parts = []
            for i in range(2):
                row = jnp.broadcast_to(crow_ref[a + i][None], (block // 16, 16, LANES)).reshape(block, LANES)
                parts.append(ones_where(cs - row < INSIDE))
            part = mm(jnp.concatenate(parts, axis=1), xcat_ref[a * LANES : (a + 2) * LANES, :])
            both = part if both is None else both + part
        sums_ref[pl.ds(base, block), :] = both[:, :LANES] + both[:, LANES:]
        return carry

    lax.fori_loop(first_j, last_j, step, 0)


def whole_kernel(
    nodes, most, group, rows_ref, mask_ref, keys_ref, gains_ref, got_ref,
    x_ref, m_ref, key_ref, gain_ref, tail_ref, tailin_ref, xcat_ref, crow_ref, c_ref, hits_ref, picks_ref,
    cs_ref, empty_ref, sums_ref, y_ref, sq_ref, sqin_ref,
    load_sems, tail_send, tail_recv, swap_send, swap_recv, send_sem, recv_sem,
):
    me, rep = lax.axis_index("tm"), lax.axis_index("rep")
    barrier = pltpu.get_barrier_semaphore()
    size_rows = x_ref.shape[0]
    first = (size_rows // 2 - WINDOW) // LANES
    early, late = slice(0, first * LANES), slice(first * LANES, size_rows)
    pairs = (
        (mask_ref, m_ref),
        (rows_ref.at[late, :], x_ref.at[late, :]),
        (keys_ref, key_ref),
        (rows_ref.at[early, :], x_ref.at[early, :]),
        (gains_ref, gain_ref),
    )
    loads = [pltpu.make_async_copy(source, target, load_sems.at[i]) for i, (source, target) in enumerate(pairs)]
    for i in (0, 1, 2, 4):
        loads[i].start()

    def greet(k, carry):
        pl.semaphore_signal(barrier, inc=1, device_id=(lax.rem(me + k, nodes), rep), device_id_type=MESH)
        return carry

    pl.semaphore_signal(barrier, inc=1, device_id=(me, 1 - rep), device_id_type=MESH)
    lax.fori_loop(1, nodes, greet, 0)
    loads[0].wait()
    tail_part = find_tail(first, x_ref, m_ref[...], tail_ref, xcat_ref, crow_ref, c_ref, loads[1].wait)

    def onward(h):
        return pltpu.make_async_remote_copy(
            src_ref=tail_ref.at[h],
            dst_ref=tailin_ref.at[h],
            send_sem=tail_send.at[h],
            recv_sem=tail_recv.at[h],
            device_id=(lax.rem(me + 1, nodes), rep),
            device_id_type=MESH,
        )

    for h in range(TAIL_PARTS):
        tail_part(h)
        if h == 0:
            pl.semaphore_wait(barrier, nodes)
        if h == TAIL_PARTS - 1:
            loads[3].start()
            loads[2].wait()
        onward(h).start()
    find_slots(most, group, c_ref, key_ref, cs_ref, empty_ref, hits_ref, picks_ref)
    loads[3].wait()
    split_rows(x_ref, xcat_ref, early)
    size = group * most
    groups = nodes // group

    def place_of(j):
        return lax.rem(me // group + j, groups)

    def own(first_j, last_j):
        own_sums(size, first_j, last_j, place_of, xcat_ref, crow_ref, cs_ref, sums_ref)

    own(0, groups - 1)
    for h in range(TAIL_PARTS):
        onward(h).wait()

    tail = tailin_ref[...].reshape(WINDOW, LANES)
    high = tail.astype(jnp.bfloat16)
    tailcat = jnp.concatenate([high, (tail - high.astype(jnp.float32)).astype(jnp.bfloat16)], axis=1)
    lanes = iota((most, LANES), 1)
    loads[4].wait()
    gain = gain_ref[...]

    def swap(j):
        return pltpu.make_async_remote_copy(
            src_ref=sq_ref.at[j],
            dst_ref=sqin_ref.at[j],
            send_sem=swap_send.at[j],
            recv_sem=swap_recv.at[j],
            device_id=(me, 1 - rep),
            device_id_type=MESH,
        )

    def add_tail(j):
        g = place_of(j)
        base = pl.multiple_of(g * size, size)
        cs = cs_ref[pl.ds(base, size), :]
        parts = [
            ones_where(cs - (iota((size, LANES), 1) + (a * LANES - WINDOW)).astype(jnp.int16) < INSIDE) for a in range(WINDOW // LANES)
        ]
        both = mm(jnp.concatenate(parts, axis=1), tailcat)
        y = sums_ref[pl.ds(base, size), :] + both[:, :LANES] + both[:, LANES:]
        y_ref[pl.ds(g * group, group)] = y.reshape(group, most, LANES)
        squares = jnp.sum(y * y, axis=1, keepdims=True)
        sq = jnp.zeros((most, LANES), jnp.float32)
        for i in range(group):
            sq = jnp.where(lanes == i, squares[i * most : (i + 1) * most, :], sq)
        sq_ref[j] = sq
        swap(j).start()

    def finish(j):
        g = place_of(j)
        swap(j).wait()
        inverse = 1.0 / jnp.sqrt((sq_ref[j] + sqin_ref[j]) / F + EPSILON)
        empty = empty_ref[g]
        for i in range(group):
            k = g * group + i
            y_ref[k] = y_ref[k] * gain * inverse[:, i : i + 1] + empty[:, i : i + 1]

        def send(i, carry):
            to = g * group + lax.rem(me + 1 + i, group)
            pltpu.make_async_remote_copy(
                src_ref=y_ref.at[to],
                dst_ref=got_ref.at[me],
                send_sem=send_sem,
                recv_sem=recv_sem,
                device_id=(to, rep),
                device_id_type=MESH,
            ).start()
            return carry

        lax.fori_loop(0, group - 1 if j == 0 else group, send, 0)

    add_tail(0)
    for j in range(1, groups - 1):
        add_tail(j)
        finish(j - 1)
    own(groups - 1, groups)
    finish(groups - 2)
    add_tail(groups - 1)
    finish(groups - 1)
    got_ref[me] = y_ref[me]
    others = pl.ds(0, nodes - 1)
    every = pltpu.make_async_remote_copy(
        src_ref=y_ref.at[others],
        dst_ref=got_ref.at[others],
        send_sem=send_sem,
        recv_sem=recv_sem,
        device_id=(me, 1 - rep),
        device_id_type=MESH,
    )
    every.wait_send()
    every.wait_recv()


def place_kernel(most, got_ref, out_ref, starts_v, starts_s, sem):
    nodes = got_ref.shape[0]
    counts = jnp.sum(jnp.where(got_ref[...] < LIMIT, 1.0, 0.0), axis=1)
    earlier = as_bf16(iota((nodes, nodes), 1) < iota((nodes, nodes), 0))
    starts = mm(earlier, counts.astype(jnp.bfloat16))
    diagonal = jnp.where(iota((nodes, LANES), 0) == iota((nodes, LANES), 1), starts, 0.0)
    starts_v[...] = jnp.sum(diagonal, axis=0, keepdims=True).astype(jnp.int32)
    copy = pltpu.make_async_copy(starts_v, starts_s, sem)
    copy.start()
    out_ref[...] = jnp.zeros_like(out_ref)
    copy.wait()

    for k in range(nodes):
        block = got_ref[k]
        out_ref[pl.ds(starts_s[0, k], most), :] = jnp.where(block < LIMIT, block, 0.0)


VMEM = pl.BlockSpec(memory_space=pltpu.VMEM)
HBM = pl.BlockSpec(memory_space=pltpu.HBM)


def call(kernel, name, outs, ins, scratch, megabytes, **settings):
    params = {"vmem_limit_bytes": megabytes << 20, **settings.pop("params", {})}
    return pl.pallas_call(
        kernel,
        out_shape=outs,
        in_specs=ins,
        out_specs=jax.tree.map(lambda _: VMEM, outs),
        scratch_shapes=scratch,
        compiler_params=pltpu.CompilerParams(**params),
        name=name,
        **settings,
    )


def local(rows, row_mask, key_bucket, gain):
    size_rows, half = rows.shape
    nodes = lax.axis_size("tm")
    most = 3 * size_rows // (4 * nodes)
    chunks = size_rows // LANES
    slots = nodes * most
    f32, bf16, i16, i32 = jnp.float32, jnp.bfloat16, jnp.int16, jnp.int32
    shape = jax.ShapeDtypeStruct
    dma = pltpu.SemaphoreType.DMA
    group = 32
    vmem = pltpu.VMEM
    in_hbm = functools.partial(pltpu.with_memory_space_constraint, memory_space=pltpu.HBM)
    got = call(
        functools.partial(whole_kernel, nodes, most, group),
        "whole",
        shape((nodes, most, half), f32),
        [HBM] * 4,
        [
            vmem((size_rows, half), f32),
            vmem((chunks, LANES), i32),
            vmem((chunks, LANES), i32),
            vmem((1, half), f32),
            vmem((TAIL_PARTS, WINDOW // TAIL_PARTS, half), f32),
            vmem((TAIL_PARTS, WINDOW // TAIL_PARTS, half), f32),
            vmem((size_rows, 2 * half), bf16),
            vmem((chunks, 16, LANES), i16),
            vmem((chunks, LANES), i32),
            vmem((nodes, size_rows), bf16),
            vmem((96, size_rows), bf16),
            vmem((slots, LANES), i16),
            vmem((nodes // group, most, LANES), f32),
            vmem((slots, half), f32),
            vmem((nodes, most, half), f32),
            vmem((nodes // group, most, LANES), f32),
            vmem((nodes // group, most, LANES), f32),
            dma((5,)),
            dma((TAIL_PARTS,)),
            dma((TAIL_PARTS,)),
            dma((nodes // group,)),
            dma((nodes // group,)),
            dma,
            dma,
        ],
        40,
        params={"collective_id": 0, "has_side_effects": True},
    )(
        in_hbm(rows),
        in_hbm(row_mask.reshape(chunks, LANES)),
        in_hbm(key_bucket.reshape(chunks, LANES)),
        in_hbm(gain.reshape(1, half)),
    )
    return call(
        functools.partial(place_kernel, most),
        "place",
        shape((slots, half), f32),
        [VMEM],
        [pltpu.VMEM((1, LANES), i32), pltpu.SMEM((1, LANES), i32), dma],
        20,
    )(got)


def solution(mesh):
    in_specs = (P("tm", "rep"), P("tm"), P("tm"), P("rep"))
    out_specs = P("tm", "rep")
    return jax.shard_map(local, mesh=mesh, in_specs=in_specs, out_specs=out_specs, check_vma=False)
```

```python
import functools

import jax
import jax.numpy as jnp
from jax import lax
from jax.experimental import pallas as pl
from jax.experimental.pallas import tpu as pltpu
from jax.sharding import PartitionSpec as P

F = 256
WINDOW = 512
LANES = 128
EPSILON = 1e-06
TAIL_PARTS = 1
MESH = pl.DeviceIdType.MESH

BIAS = 32768
INSIDE = WINDOW - BIAS
NOT_LIVE = 16384
EMPTY_SLOT = 16384
EMPTY = 1e9
LIMIT = 1e8


def iota(shape, dim):
    return lax.broadcasted_iota(jnp.int32, shape, dim)


def as_bf16(test):
    return jnp.where(test, jnp.float32(1.0), jnp.float32(0.0)).astype(jnp.bfloat16)


def ones_where(test):
    return jnp.where(test, jnp.bfloat16(1.0), jnp.bfloat16(0.0))


def mm(a, b):
    return jnp.dot(a, b, preferred_element_type=jnp.float32)


def split_rows(x_ref, xcat_ref, rows):
    x = x_ref[rows, :]
    high = x.astype(jnp.bfloat16)
    xcat_ref[rows, :LANES] = high
    xcat_ref[rows, LANES:] = (x - high.astype(jnp.float32)).astype(jnp.bfloat16)


def find_tail(first, x_ref, mask, tail_ref, xcat_ref, crow_ref, c_ref, wait_rows):
    size_rows = xcat_ref.shape[0]
    chunks = size_rows // LANES
    mask_bf = mask.astype(jnp.float32).astype(jnp.bfloat16)
    upper = as_bf16(iota((LANES, LANES), 0) <= iota((LANES, LANES), 1))
    within = mm(mask_bf, upper)
    totals = mm(mask_bf, jnp.ones((LANES, LANES), jnp.bfloat16))
    below = as_bf16(iota((chunks, chunks), 1) < iota((chunks, chunks), 0))
    before = mm(below, totals.astype(jnp.bfloat16))
    count = (before + totals)[chunks - 1 : chunks, :].astype(jnp.int32)
    c = jnp.where(mask == 1, (within + before - 1.0).astype(jnp.int32), NOT_LIVE)
    c_ref[...] = c
    rows16 = [jnp.broadcast_to(c[a : a + 1, :], (16, LANES)).astype(jnp.int16) for a in range(chunks)]
    for a in range(chunks):
        crow_ref[a] = rows16[a]
    wait_rows()
    split_rows(x_ref, xcat_ref, slice(first * LANES, size_rows))
    size = WINDOW // TAIL_PARTS

    def part(h):
        wanted = jnp.broadcast_to(count - WINDOW + h * size, (size, LANES)) + iota((size, LANES), 0)
        wanted = wanted.astype(jnp.int16)
        parts = []
        for a in range(first, chunks):
            parts.append(ones_where(wanted == jnp.broadcast_to(rows16[a][None], (size // 16, 16, LANES)).reshape(size, LANES)))
        both = mm(jnp.concatenate(parts, axis=1), xcat_ref[first * LANES :, :])
        tail_ref[h] = both[:, :LANES] + both[:, LANES:]

    return part


def find_slots(most, group, c_ref, key_ref, cs_ref, empty_ref, hits_ref, picks_ref):
    chunks = c_ref.shape[0]
    c = c_ref[...]
    key = jnp.where(c < NOT_LIVE, key_ref[...], -1)
    buckets = iota((LANES, LANES), 0)
    for a in range(chunks):
        hits_ref[:, a * LANES : (a + 1) * LANES] = as_bf16(jnp.broadcast_to(key[a : a + 1, :], (LANES, LANES)) == buckets)
    upper = as_bf16(iota((256, 256), 0) <= iota((256, 256), 1))
    carry = jnp.zeros((LANES, 1), jnp.float32)
    ranks = iota((32, LANES), 0)
    for b in range(chunks // 2):
        hits = hits_ref[:, b * 256 : (b + 1) * 256]
        running = mm(hits, upper)
        rank = jnp.sum(hits.astype(jnp.float32) * (running + carry), axis=0, keepdims=True) - 1.0
        carry = carry + running[:, 255:256]
        for h in range(2):
            a = 2 * b + h
            same = jnp.broadcast_to(rank[:, h * LANES : (h + 1) * LANES], (32, LANES)).astype(jnp.int32) == ranks
            high = jnp.broadcast_to((c[a : a + 1, :] >> 6).astype(jnp.float32), (32, LANES))
            low = jnp.broadcast_to((c[a : a + 1, :] & 63).astype(jnp.float32), (32, LANES))
            place = slice(a * LANES, (a + 1) * LANES)
            picks_ref[0:32, place] = jnp.where(same, high, 0.0).astype(jnp.bfloat16)
            picks_ref[32:64, place] = jnp.where(same, low, 0.0).astype(jnp.bfloat16)
            picks_ref[64:96, place] = jnp.where(same, 1.0, 0.0).astype(jnp.bfloat16)
    found = lax.dot_general(picks_ref[...], hits_ref[...], (((1,), (1,)), ((), ())), preferred_element_type=jnp.float32)
    filled = found[64:96, :] > 0.5
    slots = found[0:32, :] * 64.0 + found[32:64, :]
    slots = jnp.where(filled, slots.astype(jnp.int32) - BIAS, EMPTY_SLOT)
    empty = jnp.where(filled, 0.0, EMPTY)[:most, :]
    for g in range(LANES // group):
        empty_ref[g] = pltpu.roll(empty, (LANES - g * group) % LANES, 1) if g else empty
    for k in range(0, LANES, 2):
        pair = [jnp.broadcast_to(slots[:most, k + j : k + j + 1], (most, LANES)) for j in range(2)]
        cs_ref[k * most : (k + 2) * most, :] = jnp.concatenate(pair, axis=0).astype(jnp.int16)


def own_sums(block, first_j, last_j, place_of, xcat_ref, crow_ref, cs_ref, sums_ref):
    chunks = crow_ref.shape[0]

    def step(j, carry):
        base = pl.multiple_of(place_of(j) * block, block)
        cs = cs_ref[pl.ds(base, block), :]
        both = None
        for a in range(0, chunks, 2):
            parts = []
            for i in range(2):
                row = jnp.broadcast_to(crow_ref[a + i][None], (block // 16, 16, LANES)).reshape(block, LANES)
                parts.append(ones_where(cs - row < INSIDE))
            part = mm(jnp.concatenate(parts, axis=1), xcat_ref[a * LANES : (a + 2) * LANES, :])
            both = part if both is None else both + part
        sums_ref[pl.ds(base, block), :] = both[:, :LANES] + both[:, LANES:]
        return carry

    lax.fori_loop(first_j, last_j, step, 0)


def whole_kernel(
    nodes, most, group, rows_ref, mask_ref, keys_ref, gains_ref, got_ref,
    x_ref, m_ref, key_ref, gain_ref, tail_ref, tailin_ref, xcat_ref, crow_ref, c_ref, hits_ref, picks_ref,
    cs_ref, empty_ref, sums_ref, y_ref, sq_ref, sqin_ref,
    load_sems, tail_send, tail_recv, swap_send, swap_recv, send_sem, recv_sem,
):
    me, rep = lax.axis_index("tm"), lax.axis_index("rep")
    barrier = pltpu.get_barrier_semaphore()
    size_rows = x_ref.shape[0]
    first = (size_rows // 2 - WINDOW) // LANES
    early, late = slice(0, first * LANES), slice(first * LANES, size_rows)
    pairs = (
        (mask_ref, m_ref),
        (rows_ref.at[late, :], x_ref.at[late, :]),
        (keys_ref, key_ref),
        (rows_ref.at[early, :], x_ref.at[early, :]),
        (gains_ref, gain_ref),
    )
    loads = [pltpu.make_async_copy(source, target, load_sems.at[i]) for i, (source, target) in enumerate(pairs)]
    for i in (0, 1, 2, 4):
        loads[i].start()

    def greet(k, carry):
        pl.semaphore_signal(barrier, inc=1, device_id=(lax.rem(me + k, nodes), rep), device_id_type=MESH)
        return carry

    pl.semaphore_signal(barrier, inc=1, device_id=(me, 1 - rep), device_id_type=MESH)
    lax.fori_loop(1, nodes, greet, 0)
    loads[0].wait()
    tail_part = find_tail(first, x_ref, m_ref[...], tail_ref, xcat_ref, crow_ref, c_ref, loads[1].wait)

    def onward(h):
        return pltpu.make_async_remote_copy(
            src_ref=tail_ref.at[h],
            dst_ref=tailin_ref.at[h],
            send_sem=tail_send.at[h],
            recv_sem=tail_recv.at[h],
            device_id=(lax.rem(me + 1, nodes), rep),
            device_id_type=MESH,
        )

    for h in range(TAIL_PARTS):
        tail_part(h)
        if h == 0:
            pl.semaphore_wait(barrier, nodes)
        if h == TAIL_PARTS - 1:
            loads[3].start()
            loads[2].wait()
        onward(h).start()
    find_slots(most, group, c_ref, key_ref, cs_ref, empty_ref, hits_ref, picks_ref)
    loads[3].wait()
    split_rows(x_ref, xcat_ref, early)
    size = group * most
    groups = nodes // group

    def place_of(j):
        return lax.rem(me // group + j, groups)

    def own(first_j, last_j):
        own_sums(size, first_j, last_j, place_of, xcat_ref, crow_ref, cs_ref, sums_ref)

    own(0, groups - 1)
    for h in range(TAIL_PARTS):
        onward(h).wait()

    tail = tailin_ref[...].reshape(WINDOW, LANES)
    high = tail.astype(jnp.bfloat16)
    tailcat = jnp.concatenate([high, (tail - high.astype(jnp.float32)).astype(jnp.bfloat16)], axis=1)
    lanes = iota((most, LANES), 1)
    loads[4].wait()
    gain = gain_ref[...]

    def swap(j):
        return pltpu.make_async_remote_copy(
            src_ref=sq_ref.at[j],
            dst_ref=sqin_ref.at[j],
            send_sem=swap_send.at[j],
            recv_sem=swap_recv.at[j],
            device_id=(me, 1 - rep),
            device_id_type=MESH,
        )

    def add_tail(j):
        g = place_of(j)
        base = pl.multiple_of(g * size, size)
        cs = cs_ref[pl.ds(base, size), :]
        parts = [
            ones_where(cs - (iota((size, LANES), 1) + (a * LANES - WINDOW)).astype(jnp.int16) < INSIDE) for a in range(WINDOW // LANES)
        ]
        both = mm(jnp.concatenate(parts, axis=1), tailcat)
        y = sums_ref[pl.ds(base, size), :] + both[:, :LANES] + both[:, LANES:]
        y_ref[pl.ds(g * group, group)] = y.reshape(group, most, LANES)
        squares = jnp.sum(y * y, axis=1, keepdims=True)
        sq = jnp.zeros((most, LANES), jnp.float32)
        for i in range(group):
            sq = jnp.where(lanes == i, squares[i * most : (i + 1) * most, :], sq)
        sq_ref[j] = sq
        swap(j).start()

    def finish(j):
        g = place_of(j)
        swap(j).wait()
        inverse = 1.0 / jnp.sqrt((sq_ref[j] + sqin_ref[j]) / F + EPSILON)
        empty = empty_ref[g]
        for i in range(group):
            k = g * group + i
            y_ref[k] = y_ref[k] * gain * inverse[:, i : i + 1] + empty[:, i : i + 1]

        def send(i, carry):
            to = g * group + lax.rem(me + 1 + i, group)
            pltpu.make_async_remote_copy(
                src_ref=y_ref.at[to],
                dst_ref=got_ref.at[me],
                send_sem=send_sem,
                recv_sem=recv_sem,
                device_id=(to, rep),
                device_id_type=MESH,
            ).start()
            return carry

        lax.fori_loop(0, group - 1 if j == 0 else group, send, 0)

    add_tail(0)
    for j in range(1, groups - 1):
        add_tail(j)
        finish(j - 1)
    finish(groups - 2)
    own(groups - 1, groups)
    add_tail(groups - 1)
    finish(groups - 1)
    got_ref[me] = y_ref[me]
    others = pl.ds(0, nodes - 1)
    every = pltpu.make_async_remote_copy(
        src_ref=y_ref.at[others],
        dst_ref=got_ref.at[others],
        send_sem=send_sem,
        recv_sem=recv_sem,
        device_id=(me, 1 - rep),
        device_id_type=MESH,
    )
    every.wait_send()
    every.wait_recv()


def place_kernel(most, got_ref, out_ref, starts_v, starts_s, sem):
    nodes = got_ref.shape[0]
    counts = jnp.sum(jnp.where(got_ref[...] < LIMIT, 1.0, 0.0), axis=1)
    earlier = as_bf16(iota((nodes, nodes), 1) < iota((nodes, nodes), 0))
    starts = mm(earlier, counts.astype(jnp.bfloat16))
    diagonal = jnp.where(iota((nodes, LANES), 0) == iota((nodes, LANES), 1), starts, 0.0)
    starts_v[...] = jnp.sum(diagonal, axis=0, keepdims=True).astype(jnp.int32)
    copy = pltpu.make_async_copy(starts_v, starts_s, sem)
    copy.start()
    out_ref[...] = jnp.zeros_like(out_ref)
    copy.wait()

    for k in range(nodes):
        block = got_ref[k]
        out_ref[pl.ds(starts_s[0, k], most), :] = jnp.where(block < LIMIT, block, 0.0)


VMEM = pl.BlockSpec(memory_space=pltpu.VMEM)
HBM = pl.BlockSpec(memory_space=pltpu.HBM)


def call(kernel, name, outs, ins, scratch, megabytes, **settings):
    params = {"vmem_limit_bytes": megabytes << 20, **settings.pop("params", {})}
    return pl.pallas_call(
        kernel,
        out_shape=outs,
        in_specs=ins,
        out_specs=jax.tree.map(lambda _: VMEM, outs),
        scratch_shapes=scratch,
        compiler_params=pltpu.CompilerParams(**params),
        name=name,
        **settings,
    )


def local(rows, row_mask, key_bucket, gain):
    size_rows, half = rows.shape
    nodes = lax.axis_size("tm")
    most = 3 * size_rows // (4 * nodes)
    chunks = size_rows // LANES
    slots = nodes * most
    f32, bf16, i16, i32 = jnp.float32, jnp.bfloat16, jnp.int16, jnp.int32
    shape = jax.ShapeDtypeStruct
    dma = pltpu.SemaphoreType.DMA
    group = 32
    vmem = pltpu.VMEM
    in_hbm = functools.partial(pltpu.with_memory_space_constraint, memory_space=pltpu.HBM)
    got = call(
        functools.partial(whole_kernel, nodes, most, group),
        "whole",
        shape((nodes, most, half), f32),
        [HBM] * 4,
        [
            vmem((size_rows, half), f32),
            vmem((chunks, LANES), i32),
            vmem((chunks, LANES), i32),
            vmem((1, half), f32),
            vmem((TAIL_PARTS, WINDOW // TAIL_PARTS, half), f32),
            vmem((TAIL_PARTS, WINDOW // TAIL_PARTS, half), f32),
            vmem((size_rows, 2 * half), bf16),
            vmem((chunks, 16, LANES), i16),
            vmem((chunks, LANES), i32),
            vmem((nodes, size_rows), bf16),
            vmem((96, size_rows), bf16),
            vmem((slots, LANES), i16),
            vmem((nodes // group, most, LANES), f32),
            vmem((slots, half), f32),
            vmem((nodes, most, half), f32),
            vmem((nodes // group, most, LANES), f32),
            vmem((nodes // group, most, LANES), f32),
            dma((5,)),
            dma((TAIL_PARTS,)),
            dma((TAIL_PARTS,)),
            dma((nodes // group,)),
            dma((nodes // group,)),
            dma,
            dma,
        ],
        40,
        params={"collective_id": 0, "has_side_effects": True},
    )(
        in_hbm(rows),
        in_hbm(row_mask.reshape(chunks, LANES)),
        in_hbm(key_bucket.reshape(chunks, LANES)),
        in_hbm(gain.reshape(1, half)),
    )
    return call(
        functools.partial(place_kernel, most),
        "place",
        shape((slots, half), f32),
        [VMEM],
        [pltpu.VMEM((1, LANES), i32), pltpu.SMEM((1, LANES), i32), dma],
        20,
    )(got)


def solution(mesh):
    in_specs = (P("tm", "rep"), P("tm"), P("tm"), P("rep"))
    out_specs = P("tm", "rep")
    return jax.shard_map(local, mesh=mesh, in_specs=in_specs, out_specs=out_specs, check_vma=False)
```
